32 devices in a mesh: dp: 16 (over z, y, x), mp: 2 (over core).
Axes of the slice: x: 2, y: 2, z: 4, core: 2. Of those that a mesh axis runs over, the one named last changes fastest.
Arguments:
- hidden_state: bfloat16 [32, 19, 19, 256], P('dp'), may hold values from -6 to 6
- actions: int32 [32, 2], P('dp'), may hold values from 0 to 361
- value_target: int32 [32, 2], P('dp'), may hold values from 0 to 600
- reward_target: int32 [32, 2], P('dp'), may hold values from 0 to 600
- kernel_first: float32 [3, 3, 256, 256], P(None, None, 'dp', 'mp'), may hold values from -6 to 6
- kernel_second: float32 [3, 3, 256, 256], P(None, None, 'dp', 'mp'), may hold values from -6 to 6
- head_weight: float32 [2, 256, 601], P('mp', 'dp'), may hold values from -6 to 6
- action_embed: float32 [2, 256], P('mp', 'dp'), may hold values from -6 to 6
- first_mean: float32 [3, 3, 256, 256], P(None, None, 'dp', 'mp'), may hold values from -0.00061035156 to 0.00061035156
- first_square: float32 [3, 3, 256, 256], P(None, None, 'dp', 'mp'), may hold values from 1e-09 to 1e-06
- second_mean: float32 [3, 3, 256, 256], P(None, None, 'dp', 'mp'), may hold values from -0.00061035156 to 0.00061035156
- second_square: float32 [3, 3, 256, 256], P(None, None, 'dp', 'mp'), may hold values from 1e-09 to 1e-06
- head_mean: float32 [2, 256, 601], P('mp', 'dp'), may hold values from -0.0029296875 to 0.0029296875
- head_square: float32 [2, 256, 601], P('mp', 'dp'), may hold values from 1e-08 to 1e-06
- embed_mean: float32 [2, 256], P('mp', 'dp'), may hold values from -0.0017089844 to 0.0017089844
- embed_square: float32 [2, 256], P('mp', 'dp'), may hold values from 1e-09 to 1e-06
Outputs:
- kernel_first_new: float32 [3, 3, 256, 256], P(None, None, 'dp', 'mp')
- kernel_second_new: float32 [3, 3, 256, 256], P(None, None, 'dp', 'mp')
- head_weight_new: float32 [2, 256, 601], P('mp', 'dp')
- action_embed_new: float32 [2, 256], P('mp', 'dp')
- first_mean_new: float32 [3, 3, 256, 256], P(None, None, 'dp', 'mp')
- first_square_new: float32 [3, 3, 256, 256], P(None, None, 'dp', 'mp')
- second_mean_new: float32 [3, 3, 256, 256], P(None, None, 'dp', 'mp')
- second_square_new: float32 [3, 3, 256, 256], P(None, None, 'dp', 'mp')
- head_mean_new: float32 [2, 256, 601], P('mp', 'dp')
- head_square_new: float32 [2, 256, 601], P('mp', 'dp')
- embed_mean_new: float32 [2, 256], P('mp', 'dp')
- embed_square_new: float32 [2, 256], P('mp', 'dp')
- first_grad: float32 [3, 3, 256, 256], P(None, None, 'dp', 'mp')
- second_grad: float32 [3, 3, 256, 256], P(None, None, 'dp', 'mp')
- head_grad: float32 [2, 256, 601], P('mp', 'dp')
- embed_grad: float32 [2, 256], P('mp', 'dp')
The draws below stay inside these ranges and needn't reach their ends.
Inputs may be any that keep to these rules, and one draw needn't show every extreme that they name: `actions`: the value 361 stands for a pass.
All inputs are finite; a program needn't handle non-finite values.
Results may differ from the reference program's by a relative error of at most 0.02.
Values may be sent and summed in bfloat16 or wider, within the bound.
A program may use at most 64 MiB of HBM per device.

```python
import math
import jax
import jax.numpy as jnp
from jax import lax

CHANNELS = 256
BOARD = 19
CELLS = 361
BUCKETS = 601
UNROLL = 2
TOTAL_POS = 32


def touch_ends(entries, stream_key, least, top_value):
    extent = entries.shape
    spot = [jax.random.randint(jax.random.fold_in(stream_key, axis), (), 0, extent[axis]) for axis in range(len(extent))]
    entries = entries.at[tuple(spot)].set(least)
    longest = extent.index(max(extent))
    spot[longest] = (spot[longest] + 1) % extent[longest]
    return entries.at[tuple(spot)].set(top_value)


def shard_levels(rng, shape, split, smallest, high):
    loudness, own = 1.0, jax.random.fold_in(rng, 6)
    for axis_at, shards_of in split:
        draws = jnp.exp(jax.random.uniform(jax.random.fold_in(own, axis_at), (shards_of,), jnp.float32, smallest / len(split), high / len(split)))
        loudness = loudness * jnp.repeat(draws, shape[axis_at] // shards_of).reshape([-1 if axis == axis_at else 1 for axis in range(len(shape))])
    return loudness


def noise(key, extent, scale, most, cuts=(), held_as=jnp.bfloat16):
    loudness = shard_levels(key, extent, cuts, -0.22, 0.18) if cuts else 1.0
    drawn = jax.random.normal(key, extent, jnp.float32) * scale * loudness
    return jnp.minimum(jnp.maximum(drawn, -most), most).astype(held_as)


def setup_inputs(seed: int = 0) -> dict:
    keys = jax.random.split(jax.random.key(seed), 17)
    return {
        "hidden_state": noise(keys[0], (TOTAL_POS, BOARD, BOARD, CHANNELS), 1.0, 6.0, ((0, 16),)),
        "actions": touch_ends(jax.random.randint(keys[1], (TOTAL_POS, UNROLL), 0, CELLS + 1), jax.random.fold_in(keys[1], 1), 0, CELLS).astype(jnp.int32),
        "value_target": touch_ends(jax.random.randint(keys[2], (TOTAL_POS, UNROLL), 0, BUCKETS), jax.random.fold_in(keys[2], 1), 0, BUCKETS - 1).astype(jnp.int32),
        "reward_target": touch_ends(jax.random.randint(keys[3], (TOTAL_POS, UNROLL), 0, BUCKETS), jax.random.fold_in(keys[3], 1), 0, BUCKETS - 1).astype(jnp.int32),
        "kernel_first": noise(keys[4], (3, 3, CHANNELS, CHANNELS), 1.0, 6.0, ((2, 16), (3, 2)), jnp.float32),
        "kernel_second": noise(keys[5], (3, 3, CHANNELS, CHANNELS), 1.0, 6.0, ((2, 16), (3, 2)), jnp.float32),
        "head_weight": noise(keys[6], (2, CHANNELS, BUCKETS), 1.0, 6.0, ((0, 2), (1, 16)), jnp.float32),
        "action_embed": noise(keys[7], (2, CHANNELS), 1.0, 6.0, ((0, 2), (1, 16)), jnp.float32),
        "first_mean": noise(keys[8], (3, 3, CHANNELS, CHANNELS), (1e-4), 0.00061035156, ((2, 16), (3, 2)), jnp.float32),
        "first_square": jnp.clip(jnp.exp(math.log(9.999999974752427e-07) - 6.9077553 * jax.random.uniform(keys[9], (3, 3, CHANNELS, CHANNELS), jnp.float32) ** shard_levels(keys[9], (3, 3, CHANNELS, CHANNELS), ((2, 16), (3, 2)), -0.2, 0.2)), 9.999999717180685e-10, 9.999999974752427e-07),
        "second_mean": noise(keys[10], (3, 3, CHANNELS, CHANNELS), (1e-4), 0.00061035156, ((2, 16), (3, 2)), jnp.float32),
        "second_square": jnp.clip(jnp.exp(math.log(9.999999974752427e-07) - 6.9077553 * jax.random.uniform(keys[11], (3, 3, CHANNELS, CHANNELS), jnp.float32) ** shard_levels(keys[11], (3, 3, CHANNELS, CHANNELS), ((2, 16), (3, 2)), -0.2, 0.2)), 9.999999717180685e-10, 9.999999974752427e-07),
        "head_mean": noise(keys[12], (2, CHANNELS, BUCKETS), (5e-4), 0.0029296875, ((0, 2), (1, 16)), jnp.float32),
        "head_square": jnp.clip(jnp.exp(math.log(9.999999974752427e-07) - 4.6051702 * jax.random.uniform(keys[13], (2, CHANNELS, BUCKETS), jnp.float32) ** shard_levels(keys[13], (2, CHANNELS, BUCKETS), ((0, 2), (1, 16)), -0.2, 0.2)), 9.99999993922529e-09, 9.999999974752427e-07),
        "embed_mean": noise(keys[14], (2, CHANNELS), (3e-4), 0.0017089844, ((0, 2), (1, 16)), jnp.float32),
        "embed_square": jnp.clip(jnp.exp(math.log(9.999999974752427e-07) - 6.9077553 * jax.random.uniform(keys[15], (2, CHANNELS), jnp.float32) ** shard_levels(keys[15], (2, CHANNELS), ((0, 2), (1, 16)), -0.2, 0.2)), 9.999999717180685e-10, 9.999999974752427e-07),
    }


head_scale = 4.0
soft_cap = 15.0
eps_norm = 1e-05
beta_one = 0.9
beta_two = 0.999
step_size = 0.1
eps_adam = 1e-08

def conv_apply(field, kernel, layout):
    return lax.conv_general_dilated(field, kernel, (1, 1), 'SAME', dimension_numbers=('NHWC', layout, 'NHWC'), preferred_element_type=jnp.float32)

def gate_slope(pre):
    sig = jax.nn.sigmoid(pre)
    return sig * (1.0 + pre * (1.0 - sig))

def tap_products(field, grad, field_rows):
    side = field.shape[1]
    padded = jnp.pad(field, ((0, 0), (1, 1), (1, 1), (0, 0)))
    flat_grad = grad.reshape(-1, grad.shape[3])
    blocks = []
    for offset in range(9):
        row_start = offset // 3
        col_start = offset % 3
        window = padded[:, row_start:row_start + side, col_start:col_start + side, :].reshape(-1, field.shape[3])
        if field_rows:
            blocks.append(lax.dot_general(window, flat_grad, (((0,), (0,)), ((), ())), preferred_element_type=jnp.float32))
        else:
            blocks.append(lax.dot_general(flat_grad, window, (((0,), (0,)), ((), ())), preferred_element_type=jnp.float32))
    stacked = jnp.stack(blocks)
    return stacked.reshape(3, 3, stacked.shape[1], stacked.shape[2])

def action_planes(move, board):
    cells = board * board
    plane = (lax.broadcasted_iota(jnp.int32, (move.shape[0], cells), 1) == move[:, None]).astype(jnp.float32)
    passed = (move == cells).astype(jnp.float32)
    return (plane.reshape(move.shape[0], board, board, 1), passed[:, None, None, None])

def head_backward(state, head_used, value_now, reward_now, total):
    pooled = lax.optimization_barrier(jnp.mean(state, axis=(1, 2))).astype(jnp.bfloat16)
    raw = head_scale * jnp.stack([jnp.dot(pooled, head_used[0], preferred_element_type=jnp.float32), jnp.dot(pooled, head_used[1], preferred_element_type=jnp.float32)])
    squashed = jnp.tanh(raw / soft_cap)
    raised = jnp.exp(soft_cap * squashed)
    chances = raised / lax.optimization_barrier(jnp.sum(raised, axis=2, keepdims=True))
    targets = jnp.stack([value_now, reward_now])
    picked = (lax.broadcasted_iota(jnp.int32, raw.shape, 2) == targets[:, :, None]).astype(jnp.float32)
    logit_grad = ((chances - picked) * (1.0 - squashed * squashed) / total).astype(jnp.bfloat16)
    pooled_grad = head_scale * (jnp.dot(logit_grad[0], head_used[0].T, preferred_element_type=jnp.float32) + jnp.dot(logit_grad[1], head_used[1].T, preferred_element_type=jnp.float32))
    return (pooled, logit_grad, pooled_grad)

def adam_update(param, grad, mean, square):
    mean_new = beta_one * mean + (1.0 - beta_one) * grad
    square_new = beta_two * square + (1.0 - beta_two) * grad * grad
    param_new = param - step_size * mean_new / (jnp.sqrt(square_new) + eps_adam)
    return (param_new, mean_new, square_new)

def reference(hidden_state, actions, value_target, reward_target, kernel_first, kernel_second, head_weight, action_embed, first_mean, first_square, second_mean, second_square, head_mean, head_square, embed_mean, embed_square):
    first_used = kernel_first.astype(jnp.bfloat16)
    second_used = kernel_second.astype(jnp.bfloat16)
    head_used = head_weight.astype(jnp.bfloat16)
    embed_used = action_embed.astype(jnp.bfloat16)
    board = hidden_state.shape[1]
    cells = board * board
    scale = (9.0 * CHANNELS) ** (-0.5)
    embed = embed_used.astype(jnp.float32)
    state = hidden_state.astype(jnp.float32)
    saved = []
    for position in range(UNROLL):
        plane, passed = action_planes(actions[:, position], board)
        mixed = state + plane * embed[0] + passed * embed[1]
        conv_input = mixed.astype(jnp.bfloat16)
        pre = scale * conv_apply(conv_input, first_used, 'HWIO')
        hidden = jax.nn.silu(pre).astype(jnp.bfloat16)
        summed = mixed + scale * conv_apply(hidden, second_used, 'HWOI')
        factor = lax.rsqrt(lax.optimization_barrier(jnp.mean(summed * summed, axis=(1, 2, 3), keepdims=True)) + eps_norm)
        state = summed * factor
        pooled, logit_grad, pooled_grad = head_backward(state, head_used, value_target[:, position], reward_target[:, position], TOTAL_POS)
        saved.append((plane, passed, conv_input, pre, hidden, summed, factor, pooled, logit_grad, pooled_grad))
    first_grad = jnp.zeros(kernel_first.shape, jnp.float32)
    second_grad = jnp.zeros(kernel_second.shape, jnp.float32)
    head_grad = jnp.zeros(head_weight.shape, jnp.float32)
    embed_grad = jnp.zeros(action_embed.shape, jnp.float32)
    carry = jnp.zeros(hidden_state.shape, jnp.float32)
    for position in range(UNROLL - 1, -1, -1):
        plane, passed, conv_input, pre, hidden, summed, factor, pooled, logit_grad, pooled_grad = saved[position]
        state_grad = carry + pooled_grad[:, None, None, :] / cells
        summed_grad = factor * state_grad - factor * factor * factor * summed * lax.optimization_barrier(jnp.mean(state_grad * summed, axis=(1, 2, 3), keepdims=True))
        branch_grad = summed_grad.astype(jnp.bfloat16)
        hidden_grad = scale * conv_apply(branch_grad, second_used[::-1, ::-1], 'HWIO')
        inner_grad = (hidden_grad * gate_slope(pre)).astype(jnp.bfloat16)
        carry = summed_grad + scale * conv_apply(inner_grad, first_used[::-1, ::-1], 'HWOI')
        first_grad = first_grad + scale * tap_products(conv_input, inner_grad, True)
        second_grad = second_grad + scale * tap_products(hidden, branch_grad, False)
        head_grad = head_grad + head_scale * jnp.stack([lax.dot_general(pooled, logit_grad[0], (((0,), (0,)), ((), ())), preferred_element_type=jnp.float32), lax.dot_general(pooled, logit_grad[1], (((0,), (0,)), ((), ())), preferred_element_type=jnp.float32)])
        embed_grad = embed_grad + jnp.stack([lax.optimization_barrier(jnp.sum(plane * carry, axis=(0, 1, 2))), lax.optimization_barrier(jnp.sum(passed * carry, axis=(0, 1, 2)))])
    first_new, first_mean_new, first_square_new = adam_update(kernel_first, first_grad, first_mean, first_square)
    second_new, second_mean_new, second_square_new = adam_update(kernel_second, second_grad, second_mean, second_square)
    head_new, head_mean_new, head_square_new = adam_update(head_weight, head_grad, head_mean, head_square)
    embed_new, embed_mean_new, embed_square_new = adam_update(action_embed, embed_grad, embed_mean, embed_square)
    return (first_new, second_new, head_new, embed_new, first_mean_new, first_square_new, second_mean_new, second_square_new, head_mean_new, head_square_new, embed_mean_new, embed_square_new, first_grad, second_grad, head_grad, embed_grad)
```

```python
import functools

import jax
import jax.numpy as jnp
from jax import lax
from jax.experimental import pallas as pl
from jax.experimental.pallas import tpu as pltpu
from jax.sharding import PartitionSpec as P

CHANNELS = 256


head_scale = 4.0
soft_cap = 15.0
eps_norm = 1e-05
beta_one = 0.9
beta_two = 0.999
step_size = 0.1
eps_adam = 1e-08


def conv_apply(field, kernel, layout):
    return lax.conv_general_dilated(
        field,
        kernel,
        (1, 1),
        "SAME",
        dimension_numbers=("NHWC", layout, "NHWC"),
        preferred_element_type=jnp.float32,
    )


def gate_slope(pre):
    sig = jax.nn.sigmoid(pre)
    return sig * (1.0 + pre * (1.0 - sig))


def tap_products(field, grad, field_rows):
    side = field.shape[1]
    padded = jnp.pad(field, ((0, 0), (1, 1), (1, 1), (0, 0)))
    flat_grad = grad.reshape(-1, grad.shape[3])
    blocks = []
    for offset in range(9):
        row_start = offset // 3
        col_start = offset % 3
        window = padded[:, row_start : row_start + side, col_start : col_start + side, :].reshape(
            -1, field.shape[3]
        )
        if field_rows:
            blocks.append(
                lax.dot_general(
                    window, flat_grad, (((0,), (0,)), ((), ())), preferred_element_type=jnp.float32
                )
            )
        else:
            blocks.append(
                lax.dot_general(
                    flat_grad, window, (((0,), (0,)), ((), ())), preferred_element_type=jnp.float32
                )
            )
    stacked = jnp.stack(blocks)
    return stacked.reshape(3, 3, stacked.shape[1], stacked.shape[2])


def action_planes(move, board):
    cells = board * board
    plane = (lax.broadcasted_iota(jnp.int32, (move.shape[0], cells), 1) == move[:, None]).astype(
        jnp.float32
    )
    passed = (move == cells).astype(jnp.float32)
    return (plane.reshape(move.shape[0], board, board, 1), passed[:, None, None, None])


def head_backward(state, head_used, value_now, reward_now, total):
    pooled = jnp.mean(state, axis=(1, 2)).astype(jnp.bfloat16)
    raw = head_scale * jnp.stack(
        [
            jnp.dot(pooled, head_used[0], preferred_element_type=jnp.float32),
            jnp.dot(pooled, head_used[1], preferred_element_type=jnp.float32),
        ]
    )
    squashed = jnp.tanh(raw / soft_cap)
    raised = jnp.exp(soft_cap * squashed)
    chances = raised / jnp.sum(raised, axis=2, keepdims=True)
    targets = jnp.stack([value_now, reward_now])
    picked = (lax.broadcasted_iota(jnp.int32, raw.shape, 2) == targets[:, :, None]).astype(
        jnp.float32
    )
    logit_grad = ((chances - picked) * (1.0 - squashed * squashed) / total).astype(jnp.bfloat16)
    pooled_grad = head_scale * (
        jnp.dot(logit_grad[0], head_used[0].T, preferred_element_type=jnp.float32)
        + jnp.dot(logit_grad[1], head_used[1].T, preferred_element_type=jnp.float32)
    )
    return (pooled, logit_grad, pooled_grad)


def adam_update(param, grad, mean, square):
    mean_new = beta_one * mean + (1.0 - beta_one) * grad
    square_new = beta_two * square + (1.0 - beta_two) * grad * grad
    param_new = param - step_size * mean_new / (jnp.sqrt(square_new) + eps_adam)
    return (param_new, mean_new, square_new)


def local_plain(
    hidden_state,
    actions,
    value_target,
    reward_target,
    kernel_first,
    kernel_second,
    head_weight,
    action_embed,
    first_mean,
    first_square,
    second_mean,
    second_square,
    head_mean,
    head_square,
    embed_mean,
    embed_square,
):
    total = hidden_state.shape[0] * lax.axis_size("dp")
    board = hidden_state.shape[1]
    cells = board * board
    scale = (9.0 * CHANNELS) ** (-0.5)
    first_used, second_used, head_used, embed_used = (
        lax.all_gather(kernel_first.astype(jnp.bfloat16), "dp", axis=2, tiled=True),
        lax.all_gather(kernel_second.astype(jnp.bfloat16), "dp", axis=2, tiled=True),
        lax.all_gather(head_weight.astype(jnp.bfloat16), "dp", axis=1, tiled=True),
        lax.all_gather(action_embed.astype(jnp.bfloat16), "dp", axis=1, tiled=True),
    )
    first_used, second_used, head_used, embed_used = (
        lax.all_gather(first_used, "mp", axis=3, tiled=True),
        lax.all_gather(second_used, "mp", axis=3, tiled=True),
        lax.all_gather(head_used, "mp", axis=0, tiled=True),
        lax.all_gather(embed_used, "mp", axis=0, tiled=True),
    )
    count = hidden_state.shape[0] // lax.axis_size("mp")
    begin = lax.axis_index("mp") * count
    states = lax.dynamic_slice_in_dim(hidden_state, begin, count, 0)
    moves = lax.dynamic_slice_in_dim(actions, begin, count, 0)
    values = lax.dynamic_slice_in_dim(value_target, begin, count, 0)
    rewards = lax.dynamic_slice_in_dim(reward_target, begin, count, 0)
    unroll = moves.shape[1]
    embed = embed_used.astype(jnp.float32)
    state = states.astype(jnp.float32)
    saved = []
    for position in range(unroll):
        plane, passed = action_planes(moves[:, position], board)
        mixed = state + plane * embed[0] + passed * embed[1]
        conv_input = mixed.astype(jnp.bfloat16)
        pre = scale * conv_apply(conv_input, first_used, "HWIO")
        hidden = jax.nn.silu(pre).astype(jnp.bfloat16)
        branch = conv_apply(hidden, second_used, "HWOI")
        summed = mixed + scale * branch
        factor = lax.rsqrt(jnp.mean(summed * summed, axis=(1, 2, 3), keepdims=True) + eps_norm)
        state = summed * factor
        pooled, logit_grad, pooled_grad = head_backward(
            state, head_used, values[:, position], rewards[:, position], total
        )
        saved.append(
            (
                plane,
                passed,
                conv_input,
                pre,
                hidden,
                summed,
                factor,
                pooled,
                logit_grad,
                pooled_grad,
            )
        )
    first_grad = jnp.zeros(first_used.shape, jnp.float32)
    second_grad = jnp.zeros(second_used.shape, jnp.float32)
    head_grad = jnp.zeros(head_used.shape, jnp.float32)
    embed_grad = jnp.zeros(embed_used.shape, jnp.float32)
    carry = jnp.zeros(states.shape, jnp.float32)
    for position in range(unroll - 1, -1, -1):
        plane, passed, conv_input, pre, hidden, summed, factor, pooled, logit_grad, pooled_grad = (
            saved[position]
        )
        state_grad = carry + pooled_grad[:, None, None, :] / cells
        summed_grad = factor * state_grad - factor * factor * factor * summed * jnp.mean(
            state_grad * summed, axis=(1, 2, 3), keepdims=True
        )
        branch_grad = summed_grad.astype(jnp.bfloat16)
        hidden_grad = scale * conv_apply(branch_grad, second_used[::-1, ::-1], "HWIO")
        inner_grad = (hidden_grad * gate_slope(pre)).astype(jnp.bfloat16)
        input_grad = conv_apply(inner_grad, first_used[::-1, ::-1], "HWOI")
        carry = summed_grad + scale * input_grad
        first_grad = first_grad + scale * tap_products(conv_input, inner_grad, True)
        second_grad = second_grad + scale * tap_products(hidden, branch_grad, False)
        head_grad = head_grad + head_scale * jnp.stack(
            [
                lax.dot_general(
                    pooled,
                    logit_grad[0],
                    (((0,), (0,)), ((), ())),
                    preferred_element_type=jnp.float32,
                ),
                lax.dot_general(
                    pooled,
                    logit_grad[1],
                    (((0,), (0,)), ((), ())),
                    preferred_element_type=jnp.float32,
                ),
            ]
        )
        embed_grad = embed_grad + jnp.stack(
            [jnp.sum(plane * carry, axis=(0, 1, 2)), jnp.sum(passed * carry, axis=(0, 1, 2))]
        )
    first_grad, second_grad, head_grad, embed_grad = (
        lax.psum_scatter(first_grad, "mp", scatter_dimension=3, tiled=True),
        lax.psum_scatter(second_grad, "mp", scatter_dimension=3, tiled=True),
        lax.psum_scatter(head_grad, "mp", scatter_dimension=0, tiled=True),
        lax.psum_scatter(embed_grad, "mp", scatter_dimension=0, tiled=True),
    )
    first_grad, second_grad, head_grad, embed_grad = (
        lax.psum_scatter(first_grad, "dp", scatter_dimension=2, tiled=True),
        lax.psum_scatter(second_grad, "dp", scatter_dimension=2, tiled=True),
        lax.psum_scatter(head_grad, "dp", scatter_dimension=1, tiled=True),
        lax.psum_scatter(embed_grad, "dp", scatter_dimension=1, tiled=True),
    )
    first_new, first_mean_new, first_square_new = adam_update(
        kernel_first, first_grad, first_mean, first_square
    )
    second_new, second_mean_new, second_square_new = adam_update(
        kernel_second, second_grad, second_mean, second_square
    )
    head_new, head_mean_new, head_square_new = adam_update(
        head_weight, head_grad, head_mean, head_square
    )
    embed_new, embed_mean_new, embed_square_new = adam_update(
        action_embed, embed_grad, embed_mean, embed_square
    )
    return (
        first_new,
        second_new,
        head_new,
        embed_new,
        first_mean_new,
        first_square_new,
        second_mean_new,
        second_square_new,
        head_mean_new,
        head_square_new,
        embed_mean_new,
        embed_square_new,
        first_grad,
        second_grad,
        head_grad,
        embed_grad,
    )


MESH_ID = pl.DeviceIdType.MESH
LINK = jnp.bfloat16


def places(nz):
    me = lax.axis_index("dp")
    core = lax.axis_index("mp")
    z, y, x = me // 4, (me // 2) % 2, me % 2
    return z, y, x, core


def index_of(z, y, x):
    return z * 4 + y * 2 + x


def greet(nz):
    z, y, x, core = places(nz)
    barrier = pltpu.get_barrier_semaphore()
    partners = [(index_of((z + d) % nz, y, x), core) for d in range(1, nz)]
    partners += [
        (index_of(z, 1 - y, x), core),
        (index_of(z, y, 1 - x), core),
        (index_of(z, y, x), 1 - core),
    ]
    for partner in partners:
        pl.semaphore_signal(barrier, inc=1, device_id=partner, device_id_type=MESH_ID)
    pl.semaphore_wait(barrier, len(partners))


def gather_kernel(nz, ins, outs, local_sem, send_sem, recv_sem):
    z, y, x, core = places(nz)
    greet(nz)
    x_first = (True, False, False)

    def spot(which, d, near, far):
        zz = (z + d) % nz
        flip_x, flip_y = (near, far) if x_first[which] else (far, near)
        yy = 1 - y if flip_y else y
        xx = 1 - x if flip_x else x
        return zz, yy, xx

    def copy(which, slot, block, target, own):
        zz, yy, xx = block
        dst = outs[which].at[core, :, zz, yy, xx]
        return pltpu.make_async_remote_copy(
            src_ref=ins[which] if own else dst,
            dst_ref=dst,
            send_sem=send_sem.at[which, slot],
            recv_sem=recv_sem.at[which, slot],
            device_id=target,
            device_id_type=MESH_ID,
        )

    def arrival(which, slot, block, from_core):
        zz, yy, xx = block
        dst = outs[which].at[from_core, :, zz, yy, xx]
        pltpu.make_async_remote_copy(
            src_ref=dst,
            dst_ref=dst,
            send_sem=send_sem.at[which, slot],
            recv_sem=recv_sem.at[which, slot],
            device_id=(index_of(z, y, x), 1 - core),
            device_id_type=MESH_ID,
        ).wait_recv()

    started = []

    def send(which, slot, block, target, own=False):
        handle = copy(which, slot, block, target, own)
        handle.start()
        started.append(handle)

    def target_of(which, near, far):
        flip_x, flip_y = (near, far) if x_first[which] else (far, near)
        return (index_of(z, 1 - y if flip_y else y, 1 - x if flip_x else x), core)

    partner = (index_of(z, y, x), 1 - core)
    arrays = range(len(outs))
    keep = []
    for d in range(1, nz):
        for which in arrays:
            send(which, d, (z, y, x), (index_of((z + d) % nz, y, x), core), True)
    for which in arrays:
        send(which, nz, (z, y, x), target_of(which, True, False), True)
        send(which, 2 * nz, (z, y, x), target_of(which, False, True), True)
        send(which, 4 * nz, (z, y, x), partner, True)
        mine = pltpu.make_async_copy(
            ins[which], outs[which].at[core, :, z, y, x], local_sem.at[which]
        )
        mine.start()
        keep.append(mine)
    for d in range(1, nz):
        back = nz - d
        for which in arrays:
            block = spot(which, back, False, False)
            arrival(which, d, block, core)
            send(which, nz + back, block, target_of(which, True, False))
            send(which, 2 * nz + back, block, target_of(which, False, True))
            send(which, 4 * nz + back, block, partner)
    order = [0] + [nz - d for d in range(1, nz)]
    for d in order:
        for which in arrays:
            block = spot(which, d, True, False)
            arrival(which, nz + d, block, core)
            send(which, 3 * nz + d, block, target_of(which, False, True))
            send(which, 5 * nz + d, block, partner)
    for near in range(2):
        for d in order:
            for which in arrays:
                block = spot(which, d, near == 1, True)
                arrival(which, (2 + near) * nz + d, block, core)
                send(which, (6 + near) * nz + d, block, partner)
    for far in range(2):
        for near in range(2):
            for d in order:
                for which in arrays:
                    block = spot(which, d, near == 1, far == 1)
                    arrival(which, (4 + 2 * far + near) * nz + d, block, 1 - core)
    for handle in keep:
        handle.wait()
    for handle in started:
        handle.wait_send()


def gather_call(nz, blocks):
    count = len(blocks)

    def body(*refs):
        gather_kernel(nz, refs[:count], refs[count : 2 * count], *refs[2 * count :])

    vmem = pl.BlockSpec(memory_space=pltpu.VMEM)
    return pl.pallas_call(
        body,
        out_shape=[
            jax.ShapeDtypeStruct((2, b.shape[0], nz, 2, 2) + b.shape[1:], b.dtype) for b in blocks
        ],
        in_specs=[vmem] * count,
        out_specs=[vmem] * count,
        scratch_shapes=[
            pltpu.SemaphoreType.DMA((count,)),
            pltpu.SemaphoreType.DMA((count, 8 * nz)),
            pltpu.SemaphoreType.DMA((count, 8 * nz)),
        ],
        compiler_params=pltpu.CompilerParams(collective_id=0, has_side_effects=True),
        name="weights_gather",
    )(*blocks)


def reduce_kernel(nz, parts, outs, bufs, send_sem, recv_sem):
    z, y, x, core = places(nz)
    greet(nz)
    y_first = (True, False, True)
    arrays = range(len(outs))
    order = list(range(1, nz)) + [0]
    started = []

    def send(which, stage, d, src, dst, target):
        handle = pltpu.make_async_remote_copy(
            src_ref=src,
            dst_ref=dst,
            send_sem=send_sem.at[which, stage, d],
            recv_sem=recv_sem.at[which, stage, d],
            device_id=target,
            device_id_type=MESH_ID,
        )
        handle.start()
        started.append(handle)
        return handle

    handles = {}
    for d in order:
        for which in arrays:
            handles[which, 0, d] = send(
                which,
                0,
                d,
                parts[which].at[1 - core, :, (z + d) % nz],
                bufs[which][0].at[d],
                (index_of(z, y, x), 1 - core),
            )

    def first(which, d):
        got, one = bufs[which][0], bufs[which][1]
        handles[which, 0, d].wait_recv()
        for row in range(2):
            one[d, :, row] = (
                parts[which][core, :, (z + d) % nz, row].astype(jnp.float32)
                + got[d, :, row].astype(jnp.float32)
            ).astype(LINK)
        if y_first[which]:
            src, target = one.at[d, :, 1 - y], (index_of(z, 1 - y, x), core)
        else:
            src, target = one.at[d, :, :, 1 - x], (index_of(z, y, 1 - x), core)
        handles[which, 1, d] = send(which, 1, d, src, bufs[which][2].at[d], target)

    def second(which, d):
        one, got, two = bufs[which][1], bufs[which][2], bufs[which][3]
        handles[which, 1, d].wait_recv()
        own = one[d, :, y] if y_first[which] else one[d, :, :, x]
        two[d] = (own.astype(jnp.float32) + got[d].astype(jnp.float32)).astype(LINK)
        if y_first[which]:
            src, target = two.at[d, :, 1 - x], (index_of(z, y, 1 - x), core)
        else:
            src, target = two.at[d, :, 1 - y], (index_of(z, 1 - y, x), core)
        handles[which, 2, d] = send(which, 2, d, src, bufs[which][4].at[d], target)

    def third(which, d):
        two, got, three = bufs[which][3], bufs[which][4], bufs[which][5]
        handles[which, 2, d].wait_recv()
        own = two[d, :, x] if y_first[which] else two[d, :, y]
        total = own.astype(jnp.float32) + got[d].astype(jnp.float32)
        if d == 0:
            outs[which][...] = total
        else:
            three[d] = total.astype(LINK)
            handles[which, 3, d] = send(
                which,
                3,
                d,
                three.at[d],
                bufs[which][6].at[d],
                (index_of((z + d) % nz, y, x), core),
            )

    for step in range(nz + 2):
        for stage, act in enumerate((first, second, third)):
            if 0 <= step - stage < nz:
                for which in arrays:
                    act(which, order[step - stage])
    for which in arrays:
        total = outs[which][...]
        for d in range(1, nz):
            handles[which, 3, d].wait_recv()
            total = total + bufs[which][6][d].astype(jnp.float32)
        outs[which][...] = total
    for handle in started:
        handle.wait_send()


def reduce_call(nz, parts):
    count = len(parts)

    def body(*refs):
        held = refs[2 * count :]
        bufs = [held[7 * i : 7 * i + 7] for i in range(count)]
        reduce_kernel(nz, refs[:count], refs[count : 2 * count], bufs, *held[7 * count :])

    vmem = pl.BlockSpec(memory_space=pltpu.VMEM)
    scratch, shapes = [], []
    for p in parts:
        taps, rows, lanes = p.shape[1], p.shape[5], p.shape[6]
        four, two, one = (nz, taps, 2, 2, rows, lanes), (nz, taps, 2, rows, lanes), (nz, taps, rows, lanes)
        scratch += [pltpu.VMEM(s, LINK) for s in (four, four, two, two, one, one, one)]
        shapes.append(jax.ShapeDtypeStruct((taps, rows, lanes), jnp.float32))
    scratch += [pltpu.SemaphoreType.DMA((count, 4, nz)), pltpu.SemaphoreType.DMA((count, 4, nz))]
    return pl.pallas_call(
        body,
        out_shape=shapes,
        in_specs=[vmem] * count,
        out_specs=[vmem] * count,
        scratch_shapes=scratch,
        compiler_params=pltpu.CompilerParams(
            collective_id=1, has_side_effects=True, vmem_limit_bytes=60 * 2**20
        ),
        name="gradients_reduce",
    )(*parts)


def step_kernel(
    total, board, pitch, buckets, acts, values, rewards, field, first, second, heads,
    first_out, second_out, head_out,
    in_wide, hid_wide, pre_held, sum_held, state_held, carry_held, first_acc, second_acc,
    head_left, head_right, small,
):
    count, unroll = acts.shape
    rows = board * pitch
    channels = field.shape[2]
    lanes = heads.shape[3]
    cells = board * board
    scale = (9.0 * channels) ** (-0.5)
    f32 = jnp.float32

    def grid_iota(axis):
        return lax.broadcasted_iota(jnp.int32, (board, pitch, channels), axis)

    def inside():
        return (grid_iota(1) < board).reshape(rows, channels)

    def spread(value):
        return jnp.concatenate(
            [pltpu.roll(value, 1, 0), value, pltpu.roll(value, rows - 1, 0)], axis=1
        ).astype(jnp.bfloat16)

    def down(value):
        return jnp.concatenate([jnp.zeros((pitch, channels), f32), value[: rows - pitch]], axis=0)

    def up(value):
        return jnp.concatenate([value[pitch:], jnp.zeros((pitch, channels), f32)], axis=0)

    def tap(ref, offset):
        return jnp.concatenate([ref[0, offset], ref[1, offset]], axis=1)

    def conv(wide, ref, flip, turned):
        rows_out = None
        for a in (1, 0, 2):
            part = None
            for b in range(3):
                offset = 8 - (a * 3 + b) if flip else a * 3 + b
                piece = lax.dot_general(
                    wide[:, b * channels : (b + 1) * channels],
                    tap(ref, offset),
                    (((1,), (1 if turned else 0,)), ((), ())),
                    preferred_element_type=f32,
                )
                part = piece if part is None else part + piece
            if a == 0:
                part = down(part)
            elif a == 2:
                part = up(part)
            rows_out = part if rows_out is None else rows_out + part
        return jnp.where(inside(), rows_out, 0.0)

    def outer(left, right):
        return lax.dot_general(
            left, right, (((0,), (0,)), ((), ())), preferred_element_type=f32
        )

    lane = lax.broadcasted_iota(jnp.int32, (8, lanes), 1)
    row_small = lax.broadcasted_iota(jnp.int32, (8, lanes), 0)
    row_chan = lax.broadcasted_iota(jnp.int32, (8, channels), 0)
    mark = jnp.where(lane == buckets, 1.0, 0.0).astype(jnp.bfloat16)

    def head_of(h):
        return heads[h, 0]

    def lane_dot(left, right):
        return lax.dot_general(
            left, right, (((1,), (1,)), ((), ())), preferred_element_type=f32
        )

    embed = [lane_dot(mark, head_of(h))[0:1] for h in range(2)]

    first_acc[...] = jnp.zeros_like(first_acc)
    second_acc[...] = jnp.zeros_like(second_acc)

    for n in range(count):
        head_left[...] = jnp.zeros_like(head_left)
        head_right[...] = jnp.zeros_like(head_right)
        state_held[...] = field[n].astype(f32)

        def forward(k, _):
            move = acts[n, k]
            spot = jnp.where(
                grid_iota(1) < board, grid_iota(0) * board + grid_iota(1), -1
            ).reshape(rows, channels)
            passed = jnp.where(move == cells, 1.0, 0.0)
            mixed = state_held[...] + jnp.where(spot == move, embed[0], 0.0)
            mixed = mixed + jnp.where(spot >= 0, passed * embed[1], 0.0)
            sum_held[k] = mixed
            in_wide[k] = spread(mixed)
            pre = scale * conv(in_wide[k], first, False, False)
            pre_held[k] = pre
            hid_wide[k] = spread((pre * jax.nn.sigmoid(pre)).astype(jnp.bfloat16).astype(f32))
            summed = sum_held[k] + scale * conv(hid_wide[k], second, False, True)
            sum_held[k] = summed
            factor = lax.rsqrt(jnp.sum(summed * summed) / (cells * channels) + eps_norm)
            state = summed * factor
            state_held[...] = state
            pooled = (jnp.sum(state, axis=0, keepdims=True) / cells).astype(jnp.bfloat16)
            pooled8 = jnp.broadcast_to(pooled.astype(f32), (8, channels)).astype(jnp.bfloat16)
            pooled_grad = jnp.zeros((8, channels), f32)
            for h, targets in ((0, values), (1, rewards)):
                raw = head_scale * jnp.dot(pooled8, head_of(h), preferred_element_type=f32)
                squashed = jnp.tanh(raw / soft_cap)
                raised = jnp.where(lane < buckets, jnp.exp(soft_cap * squashed), 0.0)
                chances = raised / jnp.sum(raised, axis=1, keepdims=True)
                picked = jnp.where(lane == targets[n, k], 1.0, 0.0)
                grad = (chances - picked) * (1.0 - squashed * squashed) / total
                grad = jnp.where(lane < buckets, grad, 0.0)
                grad16 = grad.astype(jnp.bfloat16)
                pooled_grad = pooled_grad + lane_dot(grad16, head_of(h))
                head_right[h] = jnp.where(row_small == k, grad16.astype(f32), head_right[h])
                head_left[h] = jnp.where(row_chan == k, pooled8.astype(f32), head_left[h])
            small[k, 0] = head_scale * pooled_grad / cells
            small[k, 1] = jnp.full((8, channels), factor, f32)
            return 0

        lax.fori_loop(0, unroll, forward, 0)
        carry_held[...] = jnp.zeros_like(carry_held)

        def backward(step, sums):
            k = unroll - 1 - step
            move = acts[n, k]
            factor = small[k, 1][0:1]
            summed = sum_held[k]
            state_grad = jnp.where(inside(), carry_held[...] + small[k, 0][0:1], 0.0)
            dots = jnp.sum(state_grad * summed) / (cells * channels)
            summed_grad = factor * state_grad - factor * factor * factor * summed * dots
            state_held[...] = summed_grad
            branch = summed_grad.astype(jnp.bfloat16).astype(f32)
            hidden_grad = scale * conv(spread(branch), second, True, False)
            pre = pre_held[k]
            sig = jax.nn.sigmoid(pre)
            inner = (hidden_grad * (sig * (1.0 + pre * (1.0 - sig)))).astype(jnp.bfloat16).astype(f32)
            carry = state_held[...] + scale * conv(spread(inner), first, True, True)
            carry_held[...] = carry
            for a in range(3):
                move_rows = (up, lambda v: v, down)[a]
                inner_a = move_rows(inner).astype(jnp.bfloat16)
                branch_a = move_rows(branch).astype(jnp.bfloat16)
                for b in range(3):
                    cut = slice(b * channels, (b + 1) * channels)
                    first_acc[a * 3 + b] += outer(in_wide[k, :, cut], inner_a)
                    second_acc[a * 3 + b] += outer(branch_a, hid_wide[k, :, cut])
            spot = jnp.where(
                grid_iota(1) < board, grid_iota(0) * board + grid_iota(1), -1
            ).reshape(rows, channels)
            at_cell = jnp.sum(jnp.where(spot == move, carry, 0.0), axis=0, keepdims=True)
            at_pass = jnp.sum(carry, axis=0, keepdims=True) * jnp.where(move == cells, 1.0, 0.0)
            return sums[0] + at_cell, sums[1] + at_pass

        none = jnp.zeros((1, channels), f32)
        sums = lax.fori_loop(0, unroll, backward, (none, none))
        for h in range(2):
            left = jnp.where(row_chan == unroll, sums[h] / head_scale, head_left[h])
            right = jnp.where((row_small == unroll) & (lane == buckets), 1.0, head_right[h])
            grad = head_scale * outer(left.astype(jnp.bfloat16), right.astype(jnp.bfloat16))
            if n == 0:
                head_out[h, 0] = grad.astype(LINK)
            else:
                head_out[h, 0] = (head_out[h, 0].astype(f32) + grad).astype(LINK)
    half = channels // 2
    for offset in range(9):
        for core in range(2):
            cut = slice(core * half, (core + 1) * half)
            first_out[core, offset] = (scale * first_acc[offset, :, cut]).astype(LINK)
            second_out[core, offset] = (scale * second_acc[offset, :, cut]).astype(LINK)


def step_call(total, board, buckets, acts, values, rewards, field, first, second, heads):
    pitch = -(-(board + 1) // 8) * 8
    count, unroll = acts.shape
    channels = field.shape[3]
    lanes = heads.shape[3]
    rows = board * pitch
    field = jnp.pad(field, ((0, 0), (0, 0), (0, pitch - board), (0, 0))).reshape(count, rows, channels)
    vmem = pl.BlockSpec(memory_space=pltpu.VMEM)
    smem = pl.BlockSpec(memory_space=pltpu.SMEM)
    f32 = jnp.float32
    return pl.pallas_call(
        functools.partial(step_kernel, total, board, pitch, buckets),
        out_shape=[jax.ShapeDtypeStruct(a.shape, LINK) for a in (first, second, heads)],
        in_specs=[smem] * 3 + [vmem] * 4,
        out_specs=[vmem] * 3,
        scratch_shapes=[
            pltpu.VMEM((unroll, rows, 3 * channels), jnp.bfloat16),
            pltpu.VMEM((unroll, rows, 3 * channels), jnp.bfloat16),
            pltpu.VMEM((unroll, rows, channels), f32),
            pltpu.VMEM((unroll, rows, channels), f32),
            pltpu.VMEM((rows, channels), f32),
            pltpu.VMEM((rows, channels), f32),
            pltpu.VMEM((9, channels, channels), f32),
            pltpu.VMEM((9, channels, channels), f32),
            pltpu.VMEM((2, 8, channels), f32),
            pltpu.VMEM((2, 8, lanes), f32),
            pltpu.VMEM((unroll, 2, 8, channels), f32),
        ],
        compiler_params=pltpu.CompilerParams(vmem_limit_bytes=60 * 2**20),
        name="learner_step",
    )(acts, values, rewards, field, first, second, heads)


def local(*args):
    (hidden_state, actions, value_target, reward_target, kernel_first, kernel_second, head_weight,
     action_embed, first_mean, first_square, second_mean, second_square, head_mean, head_square,
     embed_mean, embed_square) = args
    span, cores = lax.axis_size("dp"), lax.axis_size("mp")
    slab = kernel_first.shape[2]
    if cores != 2 or span % 4 or slab % 16 or actions.shape[1] > 7:
        return local_plain(*args)
    nz = span // 4
    buckets = head_weight.shape[2]
    lanes = -(-(buckets + 1) // 128) * 128
    half = kernel_first.shape[3]
    channels = span * slab

    def pack(weights, column):
        joined = jnp.concatenate([weights, column[:, :, None]], axis=2).astype(LINK)
        return jnp.pad(joined, ((0, 0), (0, 0), (0, lanes - buckets - 1)))

    blocks = (
        kernel_first.astype(LINK).reshape(9, slab, half),
        kernel_second.astype(LINK).reshape(9, slab, half),
        pack(head_weight, action_embed),
    )
    used = gather_call(nz, blocks)
    count = hidden_state.shape[0] // cores
    begin = lax.axis_index("mp") * count

    def own(array):
        return lax.dynamic_slice_in_dim(array, begin, count, 0)

    flat = [u.reshape(2, u.shape[1], channels, u.shape[6]) for u in used]
    parts = step_call(
        hidden_state.shape[0] * span, hidden_state.shape[1], buckets,
        own(actions), own(value_target), own(reward_target), own(hidden_state), *flat,
    )
    sums = reduce_call(nz, [p.reshape(u.shape) for p, u in zip(parts, used)])
    first_grad = sums[0].reshape(kernel_first.shape)
    second_grad = sums[1].reshape(kernel_second.shape)
    head_grad = sums[2][:, :, :buckets]
    embed_grad = sums[2][:, :, buckets]
    first_new, first_mean_new, first_square_new = adam_update(
        kernel_first, first_grad, first_mean, first_square
    )
    second_new, second_mean_new, second_square_new = adam_update(
        kernel_second, second_grad, second_mean, second_square
    )
    head_new, head_mean_new, head_square_new = adam_update(
        head_weight, head_grad, head_mean, head_square
    )
    embed_new, embed_mean_new, embed_square_new = adam_update(
        action_embed, embed_grad, embed_mean, embed_square
    )
    return (
        first_new, second_new, head_new, embed_new,
        first_mean_new, first_square_new, second_mean_new, second_square_new,
        head_mean_new, head_square_new, embed_mean_new, embed_square_new,
        first_grad, second_grad, head_grad, embed_grad,
    )


def solution(mesh):
    placed = (
        P("dp", None, None, None),
        P("dp", None),
        P("dp", None),
        P("dp", None),
        P(None, None, "dp", "mp"),
        P(None, None, "dp", "mp"),
        P("mp", "dp", None),
        P("mp", "dp"),
        P(None, None, "dp", "mp"),
        P(None, None, "dp", "mp"),
        P(None, None, "dp", "mp"),
        P(None, None, "dp", "mp"),
        P("mp", "dp", None),
        P("mp", "dp", None),
        P("mp", "dp"),
        P("mp", "dp"),
    )
    return jax.shard_map(
        local,
        mesh=mesh,
        in_specs=placed,
        out_specs=(
            P(None, None, "dp", "mp"),
            P(None, None, "dp", "mp"),
            P("mp", "dp", None),
            P("mp", "dp"),
            P(None, None, "dp", "mp"),
            P(None, None, "dp", "mp"),
            P(None, None, "dp", "mp"),
            P(None, None, "dp", "mp"),
            P("mp", "dp", None),
            P("mp", "dp", None),
            P("mp", "dp"),
            P("mp", "dp"),
            P(None, None, "dp", "mp"),
            P(None, None, "dp", "mp"),
            P("mp", "dp", None),
            P("mp", "dp"),
        ),
        check_vma=False,
    )
```

```python
import functools

import jax
import jax.numpy as jnp
from jax import lax
from jax.experimental import pallas as pl
from jax.experimental.pallas import tpu as pltpu
from jax.sharding import PartitionSpec as P

CHANNELS = 256


head_scale = 4.0
soft_cap = 15.0
eps_norm = 1e-05
beta_one = 0.9
beta_two = 0.999
step_size = 0.1
eps_adam = 1e-08


def conv_apply(field, kernel, layout):
    return lax.conv_general_dilated(
        field,
        kernel,
        (1, 1),
        "SAME",
        dimension_numbers=("NHWC", layout, "NHWC"),
        preferred_element_type=jnp.float32,
    )


def gate_slope(pre):
    sig = jax.nn.sigmoid(pre)
    return sig * (1.0 + pre * (1.0 - sig))


def tap_products(field, grad, field_rows):
    side = field.shape[1]
    padded = jnp.pad(field, ((0, 0), (1, 1), (1, 1), (0, 0)))
    flat_grad = grad.reshape(-1, grad.shape[3])
    blocks = []
    for offset in range(9):
        row_start = offset // 3
        col_start = offset % 3
        window = padded[:, row_start : row_start + side, col_start : col_start + side, :].reshape(
            -1, field.shape[3]
        )
        if field_rows:
            blocks.append(
                lax.dot_general(
                    window, flat_grad, (((0,), (0,)), ((), ())), preferred_element_type=jnp.float32
                )
            )
        else:
            blocks.append(
                lax.dot_general(
                    flat_grad, window, (((0,), (0,)), ((), ())), preferred_element_type=jnp.float32
                )
            )
    stacked = jnp.stack(blocks)
    return stacked.reshape(3, 3, stacked.shape[1], stacked.shape[2])


def action_planes(move, board):
    cells = board * board
    plane = (lax.broadcasted_iota(jnp.int32, (move.shape[0], cells), 1) == move[:, None]).astype(
        jnp.float32
    )
    passed = (move == cells).astype(jnp.float32)
    return (plane.reshape(move.shape[0], board, board, 1), passed[:, None, None, None])


def head_backward(state, head_used, value_now, reward_now, total):
    pooled = jnp.mean(state, axis=(1, 2)).astype(jnp.bfloat16)
    raw = head_scale * jnp.stack(
        [
            jnp.dot(pooled, head_used[0], preferred_element_type=jnp.float32),
            jnp.dot(pooled, head_used[1], preferred_element_type=jnp.float32),
        ]
    )
    squashed = jnp.tanh(raw / soft_cap)
    raised = jnp.exp(soft_cap * squashed)
    chances = raised / jnp.sum(raised, axis=2, keepdims=True)
    targets = jnp.stack([value_now, reward_now])
    picked = (lax.broadcasted_iota(jnp.int32, raw.shape, 2) == targets[:, :, None]).astype(
        jnp.float32
    )
    logit_grad = ((chances - picked) * (1.0 - squashed * squashed) / total).astype(jnp.bfloat16)
    pooled_grad = head_scale * (
        jnp.dot(logit_grad[0], head_used[0].T, preferred_element_type=jnp.float32)
        + jnp.dot(logit_grad[1], head_used[1].T, preferred_element_type=jnp.float32)
    )
    return (pooled, logit_grad, pooled_grad)


def adam_update(param, grad, mean, square):
    mean_new = beta_one * mean + (1.0 - beta_one) * grad
    square_new = beta_two * square + (1.0 - beta_two) * grad * grad
    param_new = param - step_size * mean_new / (jnp.sqrt(square_new) + eps_adam)
    return (param_new, mean_new, square_new)


def local_plain(
    hidden_state,
    actions,
    value_target,
    reward_target,
    kernel_first,
    kernel_second,
    head_weight,
    action_embed,
    first_mean,
    first_square,
    second_mean,
    second_square,
    head_mean,
    head_square,
    embed_mean,
    embed_square,
):
    total = hidden_state.shape[0] * lax.axis_size("dp")
    board = hidden_state.shape[1]
    cells = board * board
    scale = (9.0 * CHANNELS) ** (-0.5)
    first_used, second_used, head_used, embed_used = (
        lax.all_gather(kernel_first.astype(jnp.bfloat16), "dp", axis=2, tiled=True),
        lax.all_gather(kernel_second.astype(jnp.bfloat16), "dp", axis=2, tiled=True),
        lax.all_gather(head_weight.astype(jnp.bfloat16), "dp", axis=1, tiled=True),
        lax.all_gather(action_embed.astype(jnp.bfloat16), "dp", axis=1, tiled=True),
    )
    first_used, second_used, head_used, embed_used = (
        lax.all_gather(first_used, "mp", axis=3, tiled=True),
        lax.all_gather(second_used, "mp", axis=3, tiled=True),
        lax.all_gather(head_used, "mp", axis=0, tiled=True),
        lax.all_gather(embed_used, "mp", axis=0, tiled=True),
    )
    count = hidden_state.shape[0] // lax.axis_size("mp")
    begin = lax.axis_index("mp") * count
    states = lax.dynamic_slice_in_dim(hidden_state, begin, count, 0)
    moves = lax.dynamic_slice_in_dim(actions, begin, count, 0)
    values = lax.dynamic_slice_in_dim(value_target, begin, count, 0)
    rewards = lax.dynamic_slice_in_dim(reward_target, begin, count, 0)
    unroll = moves.shape[1]
    embed = embed_used.astype(jnp.float32)
    state = states.astype(jnp.float32)
    saved = []
    for position in range(unroll):
        plane, passed = action_planes(moves[:, position], board)
        mixed = state + plane * embed[0] + passed * embed[1]
        conv_input = mixed.astype(jnp.bfloat16)
        pre = scale * conv_apply(conv_input, first_used, "HWIO")
        hidden = jax.nn.silu(pre).astype(jnp.bfloat16)
        branch = conv_apply(hidden, second_used, "HWOI")
        summed = mixed + scale * branch
        factor = lax.rsqrt(jnp.mean(summed * summed, axis=(1, 2, 3), keepdims=True) + eps_norm)
        state = summed * factor
        pooled, logit_grad, pooled_grad = head_backward(
            state, head_used, values[:, position], rewards[:, position], total
        )
        saved.append(
            (
                plane,
                passed,
                conv_input,
                pre,
                hidden,
                summed,
                factor,
                pooled,
                logit_grad,
                pooled_grad,
            )
        )
    first_grad = jnp.zeros(first_used.shape, jnp.float32)
    second_grad = jnp.zeros(second_used.shape, jnp.float32)
    head_grad = jnp.zeros(head_used.shape, jnp.float32)
    embed_grad = jnp.zeros(embed_used.shape, jnp.float32)
    carry = jnp.zeros(states.shape, jnp.float32)
    for position in range(unroll - 1, -1, -1):
        plane, passed, conv_input, pre, hidden, summed, factor, pooled, logit_grad, pooled_grad = (
            saved[position]
        )
        state_grad = carry + pooled_grad[:, None, None, :] / cells
        summed_grad = factor * state_grad - factor * factor * factor * summed * jnp.mean(
            state_grad * summed, axis=(1, 2, 3), keepdims=True
        )
        branch_grad = summed_grad.astype(jnp.bfloat16)
        hidden_grad = scale * conv_apply(branch_grad, second_used[::-1, ::-1], "HWIO")
        inner_grad = (hidden_grad * gate_slope(pre)).astype(jnp.bfloat16)
        input_grad = conv_apply(inner_grad, first_used[::-1, ::-1], "HWOI")
        carry = summed_grad + scale * input_grad
        first_grad = first_grad + scale * tap_products(conv_input, inner_grad, True)
        second_grad = second_grad + scale * tap_products(hidden, branch_grad, False)
        head_grad = head_grad + head_scale * jnp.stack(
            [
                lax.dot_general(
                    pooled,
                    logit_grad[0],
                    (((0,), (0,)), ((), ())),
                    preferred_element_type=jnp.float32,
                ),
                lax.dot_general(
                    pooled,
                    logit_grad[1],
                    (((0,), (0,)), ((), ())),
                    preferred_element_type=jnp.float32,
                ),
            ]
        )
        embed_grad = embed_grad + jnp.stack(
            [jnp.sum(plane * carry, axis=(0, 1, 2)), jnp.sum(passed * carry, axis=(0, 1, 2))]
        )
    first_grad, second_grad, head_grad, embed_grad = (
        lax.psum_scatter(first_grad, "mp", scatter_dimension=3, tiled=True),
        lax.psum_scatter(second_grad, "mp", scatter_dimension=3, tiled=True),
        lax.psum_scatter(head_grad, "mp", scatter_dimension=0, tiled=True),
        lax.psum_scatter(embed_grad, "mp", scatter_dimension=0, tiled=True),
    )
    first_grad, second_grad, head_grad, embed_grad = (
        lax.psum_scatter(first_grad, "dp", scatter_dimension=2, tiled=True),
        lax.psum_scatter(second_grad, "dp", scatter_dimension=2, tiled=True),
        lax.psum_scatter(head_grad, "dp", scatter_dimension=1, tiled=True),
        lax.psum_scatter(embed_grad, "dp", scatter_dimension=1, tiled=True),
    )
    first_new, first_mean_new, first_square_new = adam_update(
        kernel_first, first_grad, first_mean, first_square
    )
    second_new, second_mean_new, second_square_new = adam_update(
        kernel_second, second_grad, second_mean, second_square
    )
    head_new, head_mean_new, head_square_new = adam_update(
        head_weight, head_grad, head_mean, head_square
    )
    embed_new, embed_mean_new, embed_square_new = adam_update(
        action_embed, embed_grad, embed_mean, embed_square
    )
    return (
        first_new,
        second_new,
        head_new,
        embed_new,
        first_mean_new,
        first_square_new,
        second_mean_new,
        second_square_new,
        head_mean_new,
        head_square_new,
        embed_mean_new,
        embed_square_new,
        first_grad,
        second_grad,
        head_grad,
        embed_grad,
    )


MESH_ID = pl.DeviceIdType.MESH
LINK = jnp.bfloat16


def places(nz):
    me = lax.axis_index("dp")
    core = lax.axis_index("mp")
    z, y, x = me // 4, (me // 2) % 2, me % 2
    return z, y, x, core


def index_of(z, y, x):
    return z * 4 + y * 2 + x


def greet(nz):
    z, y, x, core = places(nz)
    barrier = pltpu.get_barrier_semaphore()
    partners = [(index_of((z + d) % nz, y, x), core) for d in range(1, nz)]
    partners += [
        (index_of(z, 1 - y, x), core),
        (index_of(z, y, 1 - x), core),
        (index_of(z, y, x), 1 - core),
    ]
    for partner in partners:
        pl.semaphore_signal(barrier, inc=1, device_id=partner, device_id_type=MESH_ID)
    pl.semaphore_wait(barrier, len(partners))


def gather_kernel(nz, raw, outs, ins, local_sem, send_sem, recv_sem):
    z, y, x, core = places(nz)
    ins[0][...] = raw[0][...].astype(LINK)
    ins[1][...] = raw[1][...].astype(LINK)
    _, slab, buckets = raw[2].shape
    lanes = ins[2].shape[2]
    eye = lax.broadcasted_iota(jnp.int32, (slab, slab), 0) == lax.broadcasted_iota(
        jnp.int32, (slab, slab), 1
    )
    column = jnp.sum(jnp.where(eye, raw[3][...], 0.0), axis=1, keepdims=True)
    aligned = buckets // 128 * 128
    tail = jnp.concatenate(
        [raw[2][0, :, aligned:], jnp.zeros((slab, lanes - buckets), jnp.float32)], axis=1
    )
    at = lax.broadcasted_iota(jnp.int32, tail.shape, 1) + aligned
    ins[2][0, :, :aligned] = raw[2][0, :, :aligned].astype(LINK)
    ins[2][0, :, aligned:] = jnp.where(at == buckets, column, tail).astype(LINK)
    greet(nz)
    x_first = (True, False, False)

    def spot(which, d, near, far):
        zz = (z + d) % nz
        flip_x, flip_y = (near, far) if x_first[which] else (far, near)
        yy = 1 - y if flip_y else y
        xx = 1 - x if flip_x else x
        return zz, yy, xx

    def copy(which, slot, block, target, own):
        zz, yy, xx = block
        dst = outs[which].at[core, zz, yy, xx]
        return pltpu.make_async_remote_copy(
            src_ref=ins[which] if own else dst,
            dst_ref=dst,
            send_sem=send_sem.at[which, slot],
            recv_sem=recv_sem.at[which, slot],
            device_id=target,
            device_id_type=MESH_ID,
        )

    def arrival(which, slot, block, from_core):
        zz, yy, xx = block
        dst = outs[which].at[from_core, zz, yy, xx]
        pltpu.make_async_remote_copy(
            src_ref=dst,
            dst_ref=dst,
            send_sem=send_sem.at[which, slot],
            recv_sem=recv_sem.at[which, slot],
            device_id=(index_of(z, y, x), 1 - core),
            device_id_type=MESH_ID,
        ).wait_recv()

    started = []

    def send(which, slot, block, target, own=False):
        handle = copy(which, slot, block, target, own)
        handle.start()
        started.append(handle)

    def target_of(which, near, far):
        flip_x, flip_y = (near, far) if x_first[which] else (far, near)
        return (index_of(z, 1 - y if flip_y else y, 1 - x if flip_x else x), core)

    partner = (index_of(z, y, x), 1 - core)
    arrays = range(len(outs))
    keep = []
    for d in range(1, nz):
        for which in arrays:
            send(which, d, (z, y, x), (index_of((z + d) % nz, y, x), core), True)
    for which in arrays:
        send(which, nz, (z, y, x), target_of(which, True, False), True)
        send(which, 2 * nz, (z, y, x), target_of(which, False, True), True)
        send(which, 4 * nz, (z, y, x), partner, True)
        mine = pltpu.make_async_copy(
            ins[which], outs[which].at[core, z, y, x], local_sem.at[which]
        )
        mine.start()
        keep.append(mine)
    for d in range(1, nz):
        back = nz - d
        for which in arrays:
            block = spot(which, back, False, False)
            arrival(which, d, block, core)
            send(which, nz + back, block, target_of(which, True, False))
            send(which, 2 * nz + back, block, target_of(which, False, True))
            send(which, 4 * nz + back, block, partner)
    order = [0] + [nz - d for d in range(1, nz)]
    for d in order:
        for which in arrays:
            block = spot(which, d, True, False)
            arrival(which, nz + d, block, core)
            send(which, 3 * nz + d, block, target_of(which, False, True))
            send(which, 5 * nz + d, block, partner)
    for near in range(2):
        for d in order:
            for which in arrays:
                block = spot(which, d, near == 1, True)
                arrival(which, (2 + near) * nz + d, block, core)
                send(which, (6 + near) * nz + d, block, partner)
    for far in range(2):
        for near in range(2):
            for d in order:
                for which in arrays:
                    block = spot(which, d, near == 1, far == 1)
                    arrival(which, (4 + 2 * far + near) * nz + d, block, 1 - core)
    for handle in keep:
        handle.wait()
    for handle in started:
        handle.wait_send()


def gather_call(nz, lanes, first, second, head, embed):
    shapes = [first.shape, second.shape, head.shape[:2] + (lanes,)]
    count = len(shapes)

    def body(*refs):
        gather_kernel(nz, refs[:4], refs[4:7], refs[7:10], *refs[10:])

    vmem = pl.BlockSpec(memory_space=pltpu.VMEM)
    return pl.pallas_call(
        body,
        out_shape=[
            jax.ShapeDtypeStruct((2, nz, 2, 2) + s, LINK) for s in shapes
        ],
        in_specs=[vmem] * 4,
        out_specs=[vmem] * count,
        scratch_shapes=[pltpu.VMEM(s, LINK) for s in shapes]
        + [
            pltpu.SemaphoreType.DMA((count,)),
            pltpu.SemaphoreType.DMA((count, 8 * nz)),
            pltpu.SemaphoreType.DMA((count, 8 * nz)),
        ],
        compiler_params=pltpu.CompilerParams(collective_id=0, has_side_effects=True),
        name="weights_gather",
    )(first, second, head, embed)


def reduce_kernel(nz, parts, outs, bufs, send_sem, recv_sem):
    z, y, x, core = places(nz)
    greet(nz)
    y_first = (True, False, True)
    arrays = range(len(outs))
    order = list(range(1, nz)) + [0]
    started = []

    def send(which, stage, d, src, dst, target):
        handle = pltpu.make_async_remote_copy(
            src_ref=src,
            dst_ref=dst,
            send_sem=send_sem.at[which, stage, d],
            recv_sem=recv_sem.at[which, stage, d],
            device_id=target,
            device_id_type=MESH_ID,
        )
        handle.start()
        started.append(handle)
        return handle

    handles = {}
    for d in order:
        for which in arrays:
            handles[which, 0, d] = send(
                which,
                0,
                d,
                parts[which].at[1 - core, (z + d) % nz],
                bufs[which][0].at[d],
                (index_of(z, y, x), 1 - core),
            )

    def first(which, d):
        got, one = bufs[which][0], bufs[which][1]
        handles[which, 0, d].wait_recv()
        for row in range(2):
            one[d, row] = (
                parts[which][core, (z + d) % nz, row].astype(jnp.float32)
                + got[d, row].astype(jnp.float32)
            ).astype(LINK)
        if y_first[which]:
            src, target = one.at[d, 1 - y], (index_of(z, 1 - y, x), core)
        else:
            src, target = one.at[d, :, 1 - x], (index_of(z, y, 1 - x), core)
        handles[which, 1, d] = send(which, 1, d, src, bufs[which][2].at[d], target)

    def second(which, d):
        one, got, two = bufs[which][1], bufs[which][2], bufs[which][3]
        handles[which, 1, d].wait_recv()
        own = one[d, y] if y_first[which] else one[d, :, x]
        two[d] = (own.astype(jnp.float32) + got[d].astype(jnp.float32)).astype(LINK)
        if y_first[which]:
            src, target = two.at[d, 1 - x], (index_of(z, y, 1 - x), core)
        else:
            src, target = two.at[d, 1 - y], (index_of(z, 1 - y, x), core)
        handles[which, 2, d] = send(which, 2, d, src, bufs[which][4].at[d], target)

    def third(which, d):
        two, got, three = bufs[which][3], bufs[which][4], bufs[which][5]
        handles[which, 2, d].wait_recv()
        own = two[d, x] if y_first[which] else two[d, y]
        total = own.astype(jnp.float32) + got[d].astype(jnp.float32)
        if d == 0:
            outs[which][...] = total
        else:
            three[d] = total.astype(LINK)
            handles[which, 3, d] = send(
                which,
                3,
                d,
                three.at[d],
                bufs[which][6].at[d],
                (index_of((z + d) % nz, y, x), core),
            )

    for step in range(nz + 2):
        for stage, act in enumerate((first, second, third)):
            if 0 <= step - stage < nz:
                for which in arrays:
                    act(which, order[step - stage])
    for which in arrays:
        total = outs[which][...]
        for d in range(1, nz):
            handles[which, 3, d].wait_recv()
            total = total + bufs[which][6][d].astype(jnp.float32)
        outs[which][...] = total
    for handle in started:
        handle.wait_send()


def reduce_call(nz, parts):
    count = len(parts)

    def body(*refs):
        held = refs[2 * count :]
        bufs = [held[7 * i : 7 * i + 7] for i in range(count)]
        reduce_kernel(nz, refs[:count], refs[count : 2 * count], bufs, *held[7 * count :])

    vmem = pl.BlockSpec(memory_space=pltpu.VMEM)
    scratch, shapes = [], []
    for p in parts:
        taps, rows, lanes = p.shape[4:]
        one = (nz, taps, rows, lanes)
        two, four = (nz, 2) + one[1:], (nz, 2, 2) + one[1:]
        scratch += [pltpu.VMEM(s, LINK) for s in (four, four, two, two, one, one, one)]
        shapes.append(jax.ShapeDtypeStruct((taps, rows, lanes), jnp.float32))
    scratch += [pltpu.SemaphoreType.DMA((count, 4, nz)), pltpu.SemaphoreType.DMA((count, 4, nz))]
    return pl.pallas_call(
        body,
        out_shape=shapes,
        in_specs=[vmem] * count,
        out_specs=[vmem] * count,
        scratch_shapes=scratch,
        compiler_params=pltpu.CompilerParams(
            collective_id=1, has_side_effects=True, vmem_limit_bytes=60 * 2**20
        ),
        name="gradients_reduce",
    )(*parts)


def step_kernel(
    total, board, pitch, buckets, acts, values, rewards, field, first, second, heads,
    first_out, second_out, head_out,
    in_wide, hid_wide, pre_held, sum_held, state_held, carry_held, first_acc, second_acc,
    head_left, head_right, small,
):
    unroll = acts.shape[1]
    count = field.shape[0]
    begin = lax.axis_index("mp") * count
    rows = board * pitch
    channels = field.shape[2]
    lanes = heads.shape[4]
    span, slab = first.shape[1], first.shape[3]
    cells = board * board
    scale = (9.0 * channels) ** (-0.5)
    f32 = jnp.float32

    def grid_iota(axis):
        return lax.broadcasted_iota(jnp.int32, (board, pitch, channels), axis)

    def inside():
        return (grid_iota(1) < board).reshape(rows, channels)

    def spread(value):
        return jnp.concatenate(
            [pltpu.roll(value, 1, 0), value, pltpu.roll(value, rows - 1, 0)], axis=1
        ).astype(jnp.bfloat16)

    def down(value):
        return jnp.concatenate([jnp.zeros((pitch, channels), f32), value[: rows - pitch]], axis=0)

    def up(value):
        return jnp.concatenate([value[pitch:], jnp.zeros((pitch, channels), f32)], axis=0)

    def tap(ref, offset):
        return jnp.concatenate(
            [ref[core, :, offset].reshape(channels, channels // 2) for core in range(2)], axis=1
        )

    def conv(wide, ref, flip, turned):
        rows_out = None
        for a in (1, 0, 2):
            part = None
            for b in range(3):
                offset = 8 - (a * 3 + b) if flip else a * 3 + b
                piece = lax.dot_general(
                    wide[:, b * channels : (b + 1) * channels],
                    tap(ref, offset),
                    (((1,), (1 if turned else 0,)), ((), ())),
                    preferred_element_type=f32,
                )
                part = piece if part is None else part + piece
            if a == 0:
                part = down(part)
            elif a == 2:
                part = up(part)
            rows_out = part if rows_out is None else rows_out + part
        return jnp.where(inside(), rows_out, 0.0)

    def outer(left, right):
        return lax.dot_general(
            left, right, (((0,), (0,)), ((), ())), preferred_element_type=f32
        )

    lane = lax.broadcasted_iota(jnp.int32, (8, lanes), 1)
    row_small = lax.broadcasted_iota(jnp.int32, (8, lanes), 0)
    row_chan = lax.broadcasted_iota(jnp.int32, (8, channels), 0)
    mark = jnp.where(lane == buckets, 1.0, 0.0).astype(jnp.bfloat16)

    def head_of(h):
        return heads[h].reshape(channels, lanes)

    def lane_dot(left, right):
        return lax.dot_general(
            left, right, (((1,), (1,)), ((), ())), preferred_element_type=f32
        )

    embed = [lane_dot(mark, head_of(h))[0:1] for h in range(2)]

    first_acc[...] = jnp.zeros_like(first_acc)
    second_acc[...] = jnp.zeros_like(second_acc)

    for n in range(count):
        head_left[...] = jnp.zeros_like(head_left)
        head_right[...] = jnp.zeros_like(head_right)
        state_held[...] = field[n].astype(f32)

        def forward(k, _):
            move = acts[begin + n, k]
            spot = jnp.where(
                grid_iota(1) < board, grid_iota(0) * board + grid_iota(1), -1
            ).reshape(rows, channels)
            passed = jnp.where(move == cells, 1.0, 0.0)
            mixed = state_held[...] + jnp.where(spot == move, embed[0], 0.0)
            mixed = mixed + jnp.where(spot >= 0, passed * embed[1], 0.0)
            sum_held[k] = mixed
            in_wide[k] = spread(mixed)
            pre = scale * conv(in_wide[k], first, False, False)
            pre_held[k] = pre
            hid_wide[k] = spread((pre * jax.nn.sigmoid(pre)).astype(jnp.bfloat16).astype(f32))
            summed = sum_held[k] + scale * conv(hid_wide[k], second, False, True)
            sum_held[k] = summed
            factor = lax.rsqrt(jnp.sum(summed * summed) / (cells * channels) + eps_norm)
            state = summed * factor
            state_held[...] = state
            pooled = (jnp.sum(state, axis=0, keepdims=True) / cells).astype(jnp.bfloat16)
            pooled8 = jnp.broadcast_to(pooled.astype(f32), (8, channels)).astype(jnp.bfloat16)
            pooled_grad = jnp.zeros((8, channels), f32)
            for h, targets in ((0, values), (1, rewards)):
                raw = head_scale * jnp.dot(pooled8, head_of(h), preferred_element_type=f32)
                squashed = jnp.tanh(raw / soft_cap)
                raised = jnp.where(lane < buckets, jnp.exp(soft_cap * squashed), 0.0)
                chances = raised / jnp.sum(raised, axis=1, keepdims=True)
                picked = jnp.where(lane == targets[begin + n, k], 1.0, 0.0)
                grad = (chances - picked) * (1.0 - squashed * squashed) / total
                grad = jnp.where(lane < buckets, grad, 0.0)
                grad16 = grad.astype(jnp.bfloat16)
                pooled_grad = pooled_grad + lane_dot(grad16, head_of(h))
                head_right[h] = jnp.where(row_small == k, grad16.astype(f32), head_right[h])
                head_left[h] = jnp.where(row_chan == k, pooled8.astype(f32), head_left[h])
            small[k, 0] = head_scale * pooled_grad / cells
            small[k, 1] = jnp.full((8, channels), factor, f32)
            return 0

        lax.fori_loop(0, unroll, forward, 0)
        carry_held[...] = jnp.zeros_like(carry_held)

        def backward(step, sums):
            k = unroll - 1 - step
            move = acts[begin + n, k]
            factor = small[k, 1][0:1]
            summed = sum_held[k]
            state_grad = jnp.where(inside(), carry_held[...] + small[k, 0][0:1], 0.0)
            dots = jnp.sum(state_grad * summed) / (cells * channels)
            summed_grad = factor * state_grad - factor * factor * factor * summed * dots
            state_held[...] = summed_grad
            branch = summed_grad.astype(jnp.bfloat16).astype(f32)
            hidden_grad = scale * conv(spread(branch), second, True, False)
            pre = pre_held[k]
            sig = jax.nn.sigmoid(pre)
            inner = (hidden_grad * (sig * (1.0 + pre * (1.0 - sig)))).astype(jnp.bfloat16).astype(f32)
            carry = state_held[...] + scale * conv(spread(inner), first, True, True)
            carry_held[...] = carry
            for a in range(3):
                move_rows = (up, lambda v: v, down)[a]
                inner_a = move_rows(inner).astype(jnp.bfloat16)
                branch_a = move_rows(branch).astype(jnp.bfloat16)
                for b in range(3):
                    cut = slice(b * channels, (b + 1) * channels)
                    first_acc[a * 3 + b] += outer(in_wide[k, :, cut], inner_a)
                    second_acc[a * 3 + b] += outer(branch_a, hid_wide[k, :, cut])
            spot = jnp.where(
                grid_iota(1) < board, grid_iota(0) * board + grid_iota(1), -1
            ).reshape(rows, channels)
            at_cell = jnp.sum(jnp.where(spot == move, carry, 0.0), axis=0, keepdims=True)
            at_pass = jnp.sum(carry, axis=0, keepdims=True) * jnp.where(move == cells, 1.0, 0.0)
            return sums[0] + at_cell, sums[1] + at_pass

        none = jnp.zeros((1, channels), f32)
        sums = lax.fori_loop(0, unroll, backward, (none, none))
        for h in range(2):
            left = jnp.where(row_chan == unroll, sums[h] / head_scale, head_left[h])
            right = jnp.where((row_small == unroll) & (lane == buckets), 1.0, head_right[h])
            grad = head_scale * outer(left.astype(jnp.bfloat16), right.astype(jnp.bfloat16))
            grad = grad.reshape(span, 1, slab, lanes)
            if n > 0:
                grad = grad + head_out[h].astype(f32)
            head_out[h] = grad.astype(LINK)
    half = channels // 2
    for offset in range(9):
        for core in range(2):
            cut = slice(core * half, (core + 1) * half)
            first_out[core, :, offset] = (
                (scale * first_acc[offset, :, cut]).astype(LINK).reshape(span, slab, half)
            )
            second_out[core, :, offset] = (
                (scale * second_acc[offset, :, cut]).astype(LINK).reshape(span, slab, half)
            )


def step_call(total, board, buckets, acts, values, rewards, field, first, second, heads):
    pitch = -(-(board + 1) // 8) * 8
    unroll = acts.shape[1]
    count, channels = field.shape[0], field.shape[3]
    lanes = heads.shape[4]
    rows = board * pitch
    field = jnp.pad(field, ((0, 0), (0, 0), (0, pitch - board), (0, 0))).reshape(count, rows, channels)
    vmem = pl.BlockSpec(memory_space=pltpu.VMEM)
    smem = pl.BlockSpec(memory_space=pltpu.SMEM)
    f32 = jnp.float32
    return pl.pallas_call(
        functools.partial(step_kernel, total, board, pitch, buckets),
        out_shape=[jax.ShapeDtypeStruct(a.shape, LINK) for a in (first, second, heads)],
        in_specs=[smem] * 3 + [vmem] * 4,
        out_specs=[vmem] * 3,
        scratch_shapes=[
            pltpu.VMEM((unroll, rows, 3 * channels), jnp.bfloat16),
            pltpu.VMEM((unroll, rows, 3 * channels), jnp.bfloat16),
            pltpu.VMEM((unroll, rows, channels), f32),
            pltpu.VMEM((unroll, rows, channels), f32),
            pltpu.VMEM((rows, channels), f32),
            pltpu.VMEM((rows, channels), f32),
            pltpu.VMEM((9, channels, channels), f32),
            pltpu.VMEM((9, channels, channels), f32),
            pltpu.VMEM((2, 8, channels), f32),
            pltpu.VMEM((2, 8, lanes), f32),
            pltpu.VMEM((unroll, 2, 8, channels), f32),
        ],
        compiler_params=pltpu.CompilerParams(vmem_limit_bytes=60 * 2**20),
        name="learner_step",
    )(acts, values, rewards, field, first, second, heads)


def local(*args):
    (hidden_state, actions, value_target, reward_target, kernel_first, kernel_second, head_weight,
     action_embed, first_mean, first_square, second_mean, second_square, head_mean, head_square,
     embed_mean, embed_square) = args
    span, cores = lax.axis_size("dp"), lax.axis_size("mp")
    slab = kernel_first.shape[2]
    if cores != 2 or span % 4 or slab % 16 or actions.shape[1] > 7:
        return local_plain(*args)
    nz = span // 4
    buckets = head_weight.shape[2]
    lanes = -(-(buckets + 1) // 128) * 128
    half = kernel_first.shape[3]

    used = gather_call(
        nz,
        lanes,
        kernel_first.reshape(9, slab, half),
        kernel_second.reshape(9, slab, half),
        head_weight,
        action_embed,
    )
    count = hidden_state.shape[0] // cores
    begin = lax.axis_index("mp") * count

    states = lax.dynamic_slice_in_dim(hidden_state, begin, count, 0)
    flat = [u.reshape((2, span) + u.shape[4:]) for u in used]
    parts = step_call(
        hidden_state.shape[0] * span, hidden_state.shape[1], buckets,
        actions, value_target, reward_target, states, *flat,
    )
    sums = reduce_call(nz, [p.reshape(u.shape) for p, u in zip(parts, used)])
    def flatten(array):
        return array.reshape(9, slab, half)

    outs = adam_call(
        buckets,
        *sums,
        *[flatten(a) for a in (kernel_first, first_mean, first_square)],
        *[flatten(a) for a in (kernel_second, second_mean, second_square)],
        head_weight, head_mean, head_square,
        action_embed, embed_mean, embed_square,
    )
    shaped = [o.reshape(kernel_first.shape) if o.ndim == 3 and o.shape[0] == 9 else o for o in outs]
    first, second, head, embed = (shaped[4 * i : 4 * i + 4] for i in range(4))
    return (
        first[0], second[0], head[0], embed[0],
        first[1], first[2], second[1], second[2],
        head[1], head[2], embed[1], embed[2],
        first[3], second[3], head[3], embed[3],
    )


def adam_kernel(buckets, *refs):
    sums, old, new = refs[:3], refs[3:15], refs[15:]
    slab = sums[2].shape[1]
    eye = lax.broadcasted_iota(jnp.int32, (slab, slab), 0) == lax.broadcasted_iota(
        jnp.int32, (slab, slab), 1
    )
    embed_grad = jnp.sum(
        jnp.where(eye, sums[2][0, :, buckets : buckets + 1], 0.0), axis=0, keepdims=True
    )
    grads = (sums[0][...], sums[1][...], sums[2][:, :, :buckets], embed_grad)
    for i, grad in enumerate(grads):
        param, mean, square = (old[3 * i + j][...] for j in range(3))
        made = adam_update(param, grad, mean, square) + (grad,)
        for j in range(4):
            new[4 * i + j][...] = made[j]


def adam_call(buckets, *arrays):
    vmem = pl.BlockSpec(memory_space=pltpu.VMEM)
    shapes = []
    for i in range(4):
        shapes += [jax.ShapeDtypeStruct(arrays[3 + 3 * i].shape, jnp.float32)] * 4
    return pl.pallas_call(
        functools.partial(adam_kernel, buckets),
        out_shape=shapes,
        in_specs=[vmem] * len(arrays),
        out_specs=[vmem] * len(shapes),
        name="adam",
    )(*arrays)


def solution(mesh):
    placed = (
        P("dp", None, None, None),
        P("dp", None),
        P("dp", None),
        P("dp", None),
        P(None, None, "dp", "mp"),
        P(None, None, "dp", "mp"),
        P("mp", "dp", None),
        P("mp", "dp"),
        P(None, None, "dp", "mp"),
        P(None, None, "dp", "mp"),
        P(None, None, "dp", "mp"),
        P(None, None, "dp", "mp"),
        P("mp", "dp", None),
        P("mp", "dp", None),
        P("mp", "dp"),
        P("mp", "dp"),
    )
    return jax.shard_map(
        local,
        mesh=mesh,
        in_specs=placed,
        out_specs=(
            P(None, None, "dp", "mp"),
            P(None, None, "dp", "mp"),
            P("mp", "dp", None),
            P("mp", "dp"),
            P(None, None, "dp", "mp"),
            P(None, None, "dp", "mp"),
            P(None, None, "dp", "mp"),
            P(None, None, "dp", "mp"),
            P("mp", "dp", None),
            P("mp", "dp", None),
            P("mp", "dp"),
            P("mp", "dp"),
            P(None, None, "dp", "mp"),
            P(None, None, "dp", "mp"),
            P("mp", "dp", None),
            P("mp", "dp"),
        ),
        check_vma=False,
    )
```

```python
import functools

import jax
import jax.numpy as jnp
from jax import lax
from jax.experimental import pallas as pl
from jax.experimental.pallas import tpu as pltpu
from jax.sharding import PartitionSpec as P

CHANNELS = 256


head_scale = 4.0
soft_cap = 15.0
eps_norm = 1e-05
beta_one = 0.9
beta_two = 0.999
step_size = 0.1
eps_adam = 1e-08


def conv_apply(field, kernel, layout):
    return lax.conv_general_dilated(
        field,
        kernel,
        (1, 1),
        "SAME",
        dimension_numbers=("NHWC", layout, "NHWC"),
        preferred_element_type=jnp.float32,
    )


def gate_slope(pre):
    sig = jax.nn.sigmoid(pre)
    return sig * (1.0 + pre * (1.0 - sig))


def tap_products(field, grad, field_rows):
    side = field.shape[1]
    padded = jnp.pad(field, ((0, 0), (1, 1), (1, 1), (0, 0)))
    flat_grad = grad.reshape(-1, grad.shape[3])
    blocks = []
    for offset in range(9):
        row_start = offset // 3
        col_start = offset % 3
        window = padded[:, row_start : row_start + side, col_start : col_start + side, :].reshape(
            -1, field.shape[3]
        )
        if field_rows:
            blocks.append(
                lax.dot_general(
                    window, flat_grad, (((0,), (0,)), ((), ())), preferred_element_type=jnp.float32
                )
            )
        else:
            blocks.append(
                lax.dot_general(
                    flat_grad, window, (((0,), (0,)), ((), ())), preferred_element_type=jnp.float32
                )
            )
    stacked = jnp.stack(blocks)
    return stacked.reshape(3, 3, stacked.shape[1], stacked.shape[2])


def action_planes(move, board):
    cells = board * board
    plane = (lax.broadcasted_iota(jnp.int32, (move.shape[0], cells), 1) == move[:, None]).astype(
        jnp.float32
    )
    passed = (move == cells).astype(jnp.float32)
    return (plane.reshape(move.shape[0], board, board, 1), passed[:, None, None, None])


def head_backward(state, head_used, value_now, reward_now, total):
    pooled = jnp.mean(state, axis=(1, 2)).astype(jnp.bfloat16)
    raw = head_scale * jnp.stack(
        [
            jnp.dot(pooled, head_used[0], preferred_element_type=jnp.float32),
            jnp.dot(pooled, head_used[1], preferred_element_type=jnp.float32),
        ]
    )
    squashed = jnp.tanh(raw / soft_cap)
    raised = jnp.exp(soft_cap * squashed)
    chances = raised / jnp.sum(raised, axis=2, keepdims=True)
    targets = jnp.stack([value_now, reward_now])
    picked = (lax.broadcasted_iota(jnp.int32, raw.shape, 2) == targets[:, :, None]).astype(
        jnp.float32
    )
    logit_grad = ((chances - picked) * (1.0 - squashed * squashed) / total).astype(jnp.bfloat16)
    pooled_grad = head_scale * (
        jnp.dot(logit_grad[0], head_used[0].T, preferred_element_type=jnp.float32)
        + jnp.dot(logit_grad[1], head_used[1].T, preferred_element_type=jnp.float32)
    )
    return (pooled, logit_grad, pooled_grad)


def adam_update(param, grad, mean, square):
    mean_new = beta_one * mean + (1.0 - beta_one) * grad
    square_new = beta_two * square + (1.0 - beta_two) * grad * grad
    param_new = param - step_size * mean_new / (jnp.sqrt(square_new) + eps_adam)
    return (param_new, mean_new, square_new)


def local_plain(
    hidden_state,
    actions,
    value_target,
    reward_target,
    kernel_first,
    kernel_second,
    head_weight,
    action_embed,
    first_mean,
    first_square,
    second_mean,
    second_square,
    head_mean,
    head_square,
    embed_mean,
    embed_square,
):
    total = hidden_state.shape[0] * lax.axis_size("dp")
    board = hidden_state.shape[1]
    cells = board * board
    scale = (9.0 * CHANNELS) ** (-0.5)
    first_used, second_used, head_used, embed_used = (
        lax.all_gather(kernel_first.astype(jnp.bfloat16), "dp", axis=2, tiled=True),
        lax.all_gather(kernel_second.astype(jnp.bfloat16), "dp", axis=2, tiled=True),
        lax.all_gather(head_weight.astype(jnp.bfloat16), "dp", axis=1, tiled=True),
        lax.all_gather(action_embed.astype(jnp.bfloat16), "dp", axis=1, tiled=True),
    )
    first_used, second_used, head_used, embed_used = (
        lax.all_gather(first_used, "mp", axis=3, tiled=True),
        lax.all_gather(second_used, "mp", axis=3, tiled=True),
        lax.all_gather(head_used, "mp", axis=0, tiled=True),
        lax.all_gather(embed_used, "mp", axis=0, tiled=True),
    )
    count = hidden_state.shape[0] // lax.axis_size("mp")
    begin = lax.axis_index("mp") * count
    states = lax.dynamic_slice_in_dim(hidden_state, begin, count, 0)
    moves = lax.dynamic_slice_in_dim(actions, begin, count, 0)
    values = lax.dynamic_slice_in_dim(value_target, begin, count, 0)
    rewards = lax.dynamic_slice_in_dim(reward_target, begin, count, 0)
    unroll = moves.shape[1]
    embed = embed_used.astype(jnp.float32)
    state = states.astype(jnp.float32)
    saved = []
    for position in range(unroll):
        plane, passed = action_planes(moves[:, position], board)
        mixed = state + plane * embed[0] + passed * embed[1]
        conv_input = mixed.astype(jnp.bfloat16)
        pre = scale * conv_apply(conv_input, first_used, "HWIO")
        hidden = jax.nn.silu(pre).astype(jnp.bfloat16)
        branch = conv_apply(hidden, second_used, "HWOI")
        summed = mixed + scale * branch
        factor = lax.rsqrt(jnp.mean(summed * summed, axis=(1, 2, 3), keepdims=True) + eps_norm)
        state = summed * factor
        pooled, logit_grad, pooled_grad = head_backward(
            state, head_used, values[:, position], rewards[:, position], total
        )
        saved.append(
            (
                plane,
                passed,
                conv_input,
                pre,
                hidden,
                summed,
                factor,
                pooled,
                logit_grad,
                pooled_grad,
            )
        )
    first_grad = jnp.zeros(first_used.shape, jnp.float32)
    second_grad = jnp.zeros(second_used.shape, jnp.float32)
    head_grad = jnp.zeros(head_used.shape, jnp.float32)
    embed_grad = jnp.zeros(embed_used.shape, jnp.float32)
    carry = jnp.zeros(states.shape, jnp.float32)
    for position in range(unroll - 1, -1, -1):
        plane, passed, conv_input, pre, hidden, summed, factor, pooled, logit_grad, pooled_grad = (
            saved[position]
        )
        state_grad = carry + pooled_grad[:, None, None, :] / cells
        summed_grad = factor * state_grad - factor * factor * factor * summed * jnp.mean(
            state_grad * summed, axis=(1, 2, 3), keepdims=True
        )
        branch_grad = summed_grad.astype(jnp.bfloat16)
        hidden_grad = scale * conv_apply(branch_grad, second_used[::-1, ::-1], "HWIO")
        inner_grad = (hidden_grad * gate_slope(pre)).astype(jnp.bfloat16)
        input_grad = conv_apply(inner_grad, first_used[::-1, ::-1], "HWOI")
        carry = summed_grad + scale * input_grad
        first_grad = first_grad + scale * tap_products(conv_input, inner_grad, True)
        second_grad = second_grad + scale * tap_products(hidden, branch_grad, False)
        head_grad = head_grad + head_scale * jnp.stack(
            [
                lax.dot_general(
                    pooled,
                    logit_grad[0],
                    (((0,), (0,)), ((), ())),
                    preferred_element_type=jnp.float32,
                ),
                lax.dot_general(
                    pooled,
                    logit_grad[1],
                    (((0,), (0,)), ((), ())),
                    preferred_element_type=jnp.float32,
                ),
            ]
        )
        embed_grad = embed_grad + jnp.stack(
            [jnp.sum(plane * carry, axis=(0, 1, 2)), jnp.sum(passed * carry, axis=(0, 1, 2))]
        )
    first_grad, second_grad, head_grad, embed_grad = (
        lax.psum_scatter(first_grad, "mp", scatter_dimension=3, tiled=True),
        lax.psum_scatter(second_grad, "mp", scatter_dimension=3, tiled=True),
        lax.psum_scatter(head_grad, "mp", scatter_dimension=0, tiled=True),
        lax.psum_scatter(embed_grad, "mp", scatter_dimension=0, tiled=True),
    )
    first_grad, second_grad, head_grad, embed_grad = (
        lax.psum_scatter(first_grad, "dp", scatter_dimension=2, tiled=True),
        lax.psum_scatter(second_grad, "dp", scatter_dimension=2, tiled=True),
        lax.psum_scatter(head_grad, "dp", scatter_dimension=1, tiled=True),
        lax.psum_scatter(embed_grad, "dp", scatter_dimension=1, tiled=True),
    )
    first_new, first_mean_new, first_square_new = adam_update(
        kernel_first, first_grad, first_mean, first_square
    )
    second_new, second_mean_new, second_square_new = adam_update(
        kernel_second, second_grad, second_mean, second_square
    )
    head_new, head_mean_new, head_square_new = adam_update(
        head_weight, head_grad, head_mean, head_square
    )
    embed_new, embed_mean_new, embed_square_new = adam_update(
        action_embed, embed_grad, embed_mean, embed_square
    )
    return (
        first_new,
        second_new,
        head_new,
        embed_new,
        first_mean_new,
        first_square_new,
        second_mean_new,
        second_square_new,
        head_mean_new,
        head_square_new,
        embed_mean_new,
        embed_square_new,
        first_grad,
        second_grad,
        head_grad,
        embed_grad,
    )


MESH_ID = pl.DeviceIdType.MESH
LINK = jnp.bfloat16


def places(nz):
    me = lax.axis_index("dp")
    core = lax.axis_index("mp")
    z, y, x = me // 4, (me // 2) % 2, me % 2
    return z, y, x, core


def index_of(z, y, x):
    return z * 4 + y * 2 + x


def greet(nz):
    z, y, x, core = places(nz)
    barrier = pltpu.get_barrier_semaphore()
    partners = [(index_of((z + d) % nz, y, x), core) for d in range(1, nz)]
    partners += [
        (index_of(z, 1 - y, x), core),
        (index_of(z, y, 1 - x), core),
        (index_of(z, y, x), 1 - core),
    ]
    for partner in partners:
        pl.semaphore_signal(barrier, inc=1, device_id=partner, device_id_type=MESH_ID)
    pl.semaphore_wait(barrier, len(partners))


def gather_kernel(nz, raw, outs, ins, local_sem, send_sem, recv_sem):
    z, y, x, core = places(nz)
    ins[0][...] = raw[0][...].astype(LINK)
    ins[1][...] = raw[1][...].astype(LINK)
    _, slab, buckets = raw[2].shape
    lanes = ins[2].shape[2]
    eye = lax.broadcasted_iota(jnp.int32, (slab, slab), 0) == lax.broadcasted_iota(
        jnp.int32, (slab, slab), 1
    )
    column = jnp.sum(jnp.where(eye, raw[3][...], 0.0), axis=1, keepdims=True)
    aligned = buckets // 128 * 128
    tail = jnp.concatenate(
        [raw[2][0, :, aligned:], jnp.zeros((slab, lanes - buckets), jnp.float32)], axis=1
    )
    at = lax.broadcasted_iota(jnp.int32, tail.shape, 1) + aligned
    ins[2][0, :, :aligned] = raw[2][0, :, :aligned].astype(LINK)
    ins[2][0, :, aligned:] = jnp.where(at == buckets, column, tail).astype(LINK)
    greet(nz)
    x_first = (True, False, False)

    def spot(which, d, near, far):
        zz = (z + d) % nz
        flip_x, flip_y = (near, far) if x_first[which] else (far, near)
        yy = 1 - y if flip_y else y
        xx = 1 - x if flip_x else x
        return zz, yy, xx

    def copy(which, slot, block, target, own):
        zz, yy, xx = block
        dst = outs[which].at[core, zz, yy, xx]
        return pltpu.make_async_remote_copy(
            src_ref=ins[which] if own else dst,
            dst_ref=dst,
            send_sem=send_sem.at[which, slot],
            recv_sem=recv_sem.at[which, slot],
            device_id=target,
            device_id_type=MESH_ID,
        )

    def arrival(which, slot, block, from_core):
        zz, yy, xx = block
        dst = outs[which].at[from_core, zz, yy, xx]
        pltpu.make_async_remote_copy(
            src_ref=dst,
            dst_ref=dst,
            send_sem=send_sem.at[which, slot],
            recv_sem=recv_sem.at[which, slot],
            device_id=(index_of(z, y, x), 1 - core),
            device_id_type=MESH_ID,
        ).wait_recv()

    started = []

    def send(which, slot, block, target, own=False):
        handle = copy(which, slot, block, target, own)
        handle.start()
        started.append(handle)

    def target_of(which, near, far):
        flip_x, flip_y = (near, far) if x_first[which] else (far, near)
        return (index_of(z, 1 - y if flip_y else y, 1 - x if flip_x else x), core)

    partner = (index_of(z, y, x), 1 - core)
    arrays = range(len(outs))
    keep = []
    for d in range(1, nz):
        for which in arrays:
            send(which, d, (z, y, x), (index_of((z + d) % nz, y, x), core), True)
    for which in arrays:
        send(which, nz, (z, y, x), target_of(which, True, False), True)
        send(which, 2 * nz, (z, y, x), target_of(which, False, True), True)
        send(which, 4 * nz, (z, y, x), partner, True)
        mine = pltpu.make_async_copy(
            ins[which], outs[which].at[core, z, y, x], local_sem.at[which]
        )
        mine.start()
        keep.append(mine)
    order = [0] + [nz - d for d in range(1, nz)]

    def from_z(d):
        back = nz - d
        for which in arrays:
            block = spot(which, back, False, False)
            arrival(which, d, block, core)
            send(which, nz + back, block, target_of(which, True, False))
            send(which, 2 * nz + back, block, target_of(which, False, True))
            send(which, 4 * nz + back, block, partner)

    def from_near(d):
        for which in arrays:
            block = spot(which, d, True, False)
            arrival(which, nz + d, block, core)
            send(which, 3 * nz + d, block, target_of(which, False, True))
            send(which, 5 * nz + d, block, partner)

    def from_far(near, d):
        for which in arrays:
            block = spot(which, d, near == 1, True)
            arrival(which, (2 + near) * nz + d, block, core)
            send(which, (6 + near) * nz + d, block, partner)

    from_near(0)
    for d in range(1, nz):
        from_z(d)
        if d > 1:
            from_near(order[d - 1])
        from_far(0, order[d - 1])
    if nz > 1:
        from_near(order[nz - 1])
    from_far(0, order[nz - 1])
    for d in order:
        from_far(1, d)
    for far in range(2):
        for near in range(2):
            for d in order:
                for which in arrays:
                    block = spot(which, d, near == 1, far == 1)
                    arrival(which, (4 + 2 * far + near) * nz + d, block, 1 - core)
    for handle in keep:
        handle.wait()
    for handle in started:
        handle.wait_send()


def gather_call(nz, lanes, first, second, head, embed):
    shapes = [first.shape, second.shape, head.shape[:2] + (lanes,)]
    count = len(shapes)

    def body(*refs):
        gather_kernel(nz, refs[:4], refs[4:7], refs[7:10], *refs[10:])

    vmem = pl.BlockSpec(memory_space=pltpu.VMEM)
    return pl.pallas_call(
        body,
        out_shape=[
            jax.ShapeDtypeStruct((2, nz, 2, 2) + s, LINK) for s in shapes
        ],
        in_specs=[vmem] * 4,
        out_specs=[vmem] * count,
        scratch_shapes=[pltpu.VMEM(s, LINK) for s in shapes]
        + [
            pltpu.SemaphoreType.DMA((count,)),
            pltpu.SemaphoreType.DMA((count, 8 * nz)),
            pltpu.SemaphoreType.DMA((count, 8 * nz)),
        ],
        compiler_params=pltpu.CompilerParams(collective_id=0, has_side_effects=True),
        name="weights_gather",
    )(first, second, head, embed)


def reduce_kernel(nz, parts, outs, bufs, send_sem, recv_sem):
    z, y, x, core = places(nz)
    greet(nz)
    y_first = (True, False, True)
    arrays = range(len(outs))
    order = list(range(1, nz)) + [0]
    started = []

    def send(which, stage, d, src, dst, target):
        handle = pltpu.make_async_remote_copy(
            src_ref=src,
            dst_ref=dst,
            send_sem=send_sem.at[which, stage, d],
            recv_sem=recv_sem.at[which, stage, d],
            device_id=target,
            device_id_type=MESH_ID,
        )
        handle.start()
        started.append(handle)
        return handle

    handles = {}
    for d in order:
        for which in arrays:
            handles[which, 0, d] = send(
                which,
                0,
                d,
                parts[which].at[1 - core, (z + d) % nz],
                bufs[which][0].at[d],
                (index_of(z, y, x), 1 - core),
            )

    def first(which, d):
        got, one = bufs[which][0], bufs[which][1]
        handles[which, 0, d].wait_recv()
        for row in range(2):
            one[d, row] = (
                parts[which][core, (z + d) % nz, row].astype(jnp.float32)
                + got[d, row].astype(jnp.float32)
            ).astype(LINK)
        if y_first[which]:
            src, target = one.at[d, 1 - y], (index_of(z, 1 - y, x), core)
        else:
            src, target = one.at[d, :, 1 - x], (index_of(z, y, 1 - x), core)
        handles[which, 1, d] = send(which, 1, d, src, bufs[which][2].at[d], target)

    def second(which, d):
        one, got, two = bufs[which][1], bufs[which][2], bufs[which][3]
        handles[which, 1, d].wait_recv()
        own = one[d, y] if y_first[which] else one[d, :, x]
        two[d] = (own.astype(jnp.float32) + got[d].astype(jnp.float32)).astype(LINK)
        if y_first[which]:
            src, target = two.at[d, 1 - x], (index_of(z, y, 1 - x), core)
        else:
            src, target = two.at[d, 1 - y], (index_of(z, 1 - y, x), core)
        handles[which, 2, d] = send(which, 2, d, src, bufs[which][4].at[d], target)

    def third(which, d):
        two, got, three = bufs[which][3], bufs[which][4], bufs[which][5]
        handles[which, 2, d].wait_recv()
        own = two[d, x] if y_first[which] else two[d, y]
        total = own.astype(jnp.float32) + got[d].astype(jnp.float32)
        if d == 0:
            outs[which][...] = total
        else:
            three[d] = total.astype(LINK)
            handles[which, 3, d] = send(
                which,
                3,
                d,
                three.at[d],
                bufs[which][6].at[d],
                (index_of((z + d) % nz, y, x), core),
            )

    for step in range(nz + 2):
        for stage, act in enumerate((first, second, third)):
            if 0 <= step - stage < nz:
                for which in arrays:
                    act(which, order[step - stage])
    for which in arrays:
        total = outs[which][...]
        for d in range(1, nz):
            handles[which, 3, d].wait_recv()
            total = total + bufs[which][6][d].astype(jnp.float32)
        outs[which][...] = total
    for handle in started:
        handle.wait_send()


def reduce_call(nz, parts):
    count = len(parts)

    def body(*refs):
        held = refs[2 * count :]
        bufs = [held[7 * i : 7 * i + 7] for i in range(count)]
        reduce_kernel(nz, refs[:count], refs[count : 2 * count], bufs, *held[7 * count :])

    vmem = pl.BlockSpec(memory_space=pltpu.VMEM)
    scratch, shapes = [], []
    for p in parts:
        taps, rows, lanes = p.shape[4:]
        one = (nz, taps, rows, lanes)
        two, four = (nz, 2) + one[1:], (nz, 2, 2) + one[1:]
        scratch += [pltpu.VMEM(s, LINK) for s in (four, four, two, two, one, one, one)]
        shapes.append(jax.ShapeDtypeStruct((taps, rows, lanes), jnp.float32))
    scratch += [pltpu.SemaphoreType.DMA((count, 4, nz)), pltpu.SemaphoreType.DMA((count, 4, nz))]
    return pl.pallas_call(
        body,
        out_shape=shapes,
        in_specs=[vmem] * count,
        out_specs=[vmem] * count,
        scratch_shapes=scratch,
        compiler_params=pltpu.CompilerParams(
            collective_id=1, has_side_effects=True, vmem_limit_bytes=60 * 2**20
        ),
        name="gradients_reduce",
    )(*parts)


def step_kernel(
    total, board, pitch, buckets, acts, values, rewards, field, first, second, heads,
    first_out, second_out, head_out,
    in_wide, hid_wide, pre_held, sum_held, state_held, carry_held, first_acc, second_acc,
    head_left, head_right, small,
):
    unroll = acts.shape[1]
    count = field.shape[0]
    begin = lax.axis_index("mp") * count
    rows = board * pitch
    channels = field.shape[2]
    lanes = heads.shape[4]
    span, slab = first.shape[1], first.shape[3]
    cells = board * board
    scale = (9.0 * channels) ** (-0.5)
    f32 = jnp.float32

    def grid_iota(axis):
        return lax.broadcasted_iota(jnp.int32, (board, pitch, channels), axis)

    def inside():
        return (grid_iota(1) < board).reshape(rows, channels)

    def spread(value):
        return jnp.concatenate(
            [pltpu.roll(value, 1, 0), value, pltpu.roll(value, rows - 1, 0)], axis=1
        ).astype(jnp.bfloat16)

    def down(value):
        return jnp.concatenate([jnp.zeros((pitch, channels), f32), value[: rows - pitch]], axis=0)

    def up(value):
        return jnp.concatenate([value[pitch:], jnp.zeros((pitch, channels), f32)], axis=0)

    def tap(ref, offset):
        return jnp.concatenate(
            [ref[core, :, offset].reshape(channels, channels // 2) for core in range(2)], axis=1
        )

    def conv(wide, ref, flip, turned):
        rows_out = None
        for a in (1, 0, 2):
            part = None
            for b in range(3):
                offset = 8 - (a * 3 + b) if flip else a * 3 + b
                piece = lax.dot_general(
                    wide[:, b * channels : (b + 1) * channels],
                    tap(ref, offset),
                    (((1,), (1 if turned else 0,)), ((), ())),
                    preferred_element_type=f32,
                )
                part = piece if part is None else part + piece
            if a == 0:
                part = down(part)
            elif a == 2:
                part = up(part)
            rows_out = part if rows_out is None else rows_out + part
        return jnp.where(inside(), rows_out, 0.0)

    def outer(left, right):
        return lax.dot_general(
            left, right, (((0,), (0,)), ((), ())), preferred_element_type=f32
        )

    lane = lax.broadcasted_iota(jnp.int32, (8, lanes), 1)
    row_small = lax.broadcasted_iota(jnp.int32, (8, lanes), 0)
    row_chan = lax.broadcasted_iota(jnp.int32, (8, channels), 0)
    mark = jnp.where(lane == buckets, 1.0, 0.0).astype(jnp.bfloat16)

    def head_of(h):
        return heads[h].reshape(channels, lanes)

    def lane_dot(left, right):
        return lax.dot_general(
            left, right, (((1,), (1,)), ((), ())), preferred_element_type=f32
        )

    embed = [lane_dot(mark, head_of(h))[0:1] for h in range(2)]

    first_acc[...] = jnp.zeros_like(first_acc)
    second_acc[...] = jnp.zeros_like(second_acc)

    for n in range(count):
        head_left[...] = jnp.zeros_like(head_left)
        head_right[...] = jnp.zeros_like(head_right)
        state_held[...] = field[n].astype(f32)

        def forward(k, _):
            move = acts[begin + n, k]
            spot = jnp.where(
                grid_iota(1) < board, grid_iota(0) * board + grid_iota(1), -1
            ).reshape(rows, channels)
            passed = jnp.where(move == cells, 1.0, 0.0)
            mixed = state_held[...] + jnp.where(spot == move, embed[0], 0.0)
            mixed = mixed + jnp.where(spot >= 0, passed * embed[1], 0.0)
            sum_held[k] = mixed
            in_wide[k] = spread(mixed)
            pre = scale * conv(in_wide[k], first, False, False)
            pre_held[k] = pre
            hid_wide[k] = spread((pre * jax.nn.sigmoid(pre)).astype(jnp.bfloat16).astype(f32))
            summed = sum_held[k] + scale * conv(hid_wide[k], second, False, True)
            sum_held[k] = summed
            factor = lax.rsqrt(jnp.sum(summed * summed) / (cells * channels) + eps_norm)
            state = summed * factor
            state_held[...] = state
            pooled = (jnp.sum(state, axis=0, keepdims=True) / cells).astype(jnp.bfloat16)
            pooled8 = jnp.broadcast_to(pooled.astype(f32), (8, channels)).astype(jnp.bfloat16)
            pooled_grad = jnp.zeros((8, channels), f32)
            for h, targets in ((0, values), (1, rewards)):
                raw = head_scale * jnp.dot(pooled8, head_of(h), preferred_element_type=f32)
                squashed = jnp.tanh(raw / soft_cap)
                raised = jnp.where(lane < buckets, jnp.exp(soft_cap * squashed), 0.0)
                chances = raised / jnp.sum(raised, axis=1, keepdims=True)
                picked = jnp.where(lane == targets[begin + n, k], 1.0, 0.0)
                grad = (chances - picked) * (1.0 - squashed * squashed) / total
                grad = jnp.where(lane < buckets, grad, 0.0)
                grad16 = grad.astype(jnp.bfloat16)
                pooled_grad = pooled_grad + lane_dot(grad16, head_of(h))
                head_right[h] = jnp.where(row_small == k, grad16.astype(f32), head_right[h])
                head_left[h] = jnp.where(row_chan == k, pooled8.astype(f32), head_left[h])
            small[k, 0] = head_scale * pooled_grad / cells
            small[k, 1] = jnp.full((8, channels), factor, f32)
            return 0

        lax.fori_loop(0, unroll, forward, 0)
        carry_held[...] = jnp.zeros_like(carry_held)

        def backward(step, sums):
            k = unroll - 1 - step
            move = acts[begin + n, k]
            factor = small[k, 1][0:1]
            summed = sum_held[k]
            state_grad = jnp.where(inside(), carry_held[...] + small[k, 0][0:1], 0.0)
            dots = jnp.sum(state_grad * summed) / (cells * channels)
            summed_grad = factor * state_grad - factor * factor * factor * summed * dots
            state_held[...] = summed_grad
            branch = summed_grad.astype(jnp.bfloat16).astype(f32)
            hidden_grad = scale * conv(spread(branch), second, True, False)
            pre = pre_held[k]
            sig = jax.nn.sigmoid(pre)
            inner = (hidden_grad * (sig * (1.0 + pre * (1.0 - sig)))).astype(jnp.bfloat16).astype(f32)
            carry = state_held[...] + scale * conv(spread(inner), first, True, True)
            carry_held[...] = carry
            for a in range(3):
                move_rows = (up, lambda v: v, down)[a]
                inner_a = move_rows(inner).astype(jnp.bfloat16)
                branch_a = move_rows(branch).astype(jnp.bfloat16)
                for b in range(3):
                    cut = slice(b * channels, (b + 1) * channels)
                    first_acc[a * 3 + b] += outer(in_wide[k, :, cut], inner_a)
                    second_acc[a * 3 + b] += outer(branch_a, hid_wide[k, :, cut])
            spot = jnp.where(
                grid_iota(1) < board, grid_iota(0) * board + grid_iota(1), -1
            ).reshape(rows, channels)
            at_cell = jnp.sum(jnp.where(spot == move, carry, 0.0), axis=0, keepdims=True)
            at_pass = jnp.sum(carry, axis=0, keepdims=True) * jnp.where(move == cells, 1.0, 0.0)
            return sums[0] + at_cell, sums[1] + at_pass

        none = jnp.zeros((1, channels), f32)
        sums = lax.fori_loop(0, unroll, backward, (none, none))
        for h in range(2):
            left = jnp.where(row_chan == unroll, sums[h] / head_scale, head_left[h])
            right = jnp.where((row_small == unroll) & (lane == buckets), 1.0, head_right[h])
            grad = head_scale * outer(left.astype(jnp.bfloat16), right.astype(jnp.bfloat16))
            grad = grad.reshape(span, 1, slab, lanes)
            if n > 0:
                grad = grad + head_out[h].astype(f32)
            head_out[h] = grad.astype(LINK)
    half = channels // 2
    for offset in range(9):
        for core in range(2):
            cut = slice(core * half, (core + 1) * half)
            first_out[core, :, offset] = (
                (scale * first_acc[offset, :, cut]).astype(LINK).reshape(span, slab, half)
            )
            second_out[core, :, offset] = (
                (scale * second_acc[offset, :, cut]).astype(LINK).reshape(span, slab, half)
            )


def step_call(total, board, buckets, acts, values, rewards, field, first, second, heads):
    pitch = -(-(board + 1) // 8) * 8
    unroll = acts.shape[1]
    count, channels = field.shape[0], field.shape[3]
    lanes = heads.shape[4]
    rows = board * pitch
    field = jnp.pad(field, ((0, 0), (0, 0), (0, pitch - board), (0, 0))).reshape(count, rows, channels)
    vmem = pl.BlockSpec(memory_space=pltpu.VMEM)
    smem = pl.BlockSpec(memory_space=pltpu.SMEM)
    f32 = jnp.float32
    return pl.pallas_call(
        functools.partial(step_kernel, total, board, pitch, buckets),
        out_shape=[jax.ShapeDtypeStruct(a.shape, LINK) for a in (first, second, heads)],
        in_specs=[smem] * 3 + [vmem] * 4,
        out_specs=[vmem] * 3,
        scratch_shapes=[
            pltpu.VMEM((unroll, rows, 3 * channels), jnp.bfloat16),
            pltpu.VMEM((unroll, rows, 3 * channels), jnp.bfloat16),
            pltpu.VMEM((unroll, rows, channels), f32),
            pltpu.VMEM((unroll, rows, channels), f32),
            pltpu.VMEM((rows, channels), f32),
            pltpu.VMEM((rows, channels), f32),
            pltpu.VMEM((9, channels, channels), f32),
            pltpu.VMEM((9, channels, channels), f32),
            pltpu.VMEM((2, 8, channels), f32),
            pltpu.VMEM((2, 8, lanes), f32),
            pltpu.VMEM((unroll, 2, 8, channels), f32),
        ],
        compiler_params=pltpu.CompilerParams(vmem_limit_bytes=60 * 2**20),
        name="learner_step",
    )(acts, values, rewards, field, first, second, heads)


def local(*args):
    (hidden_state, actions, value_target, reward_target, kernel_first, kernel_second, head_weight,
     action_embed, first_mean, first_square, second_mean, second_square, head_mean, head_square,
     embed_mean, embed_square) = args
    span, cores = lax.axis_size("dp"), lax.axis_size("mp")
    slab = kernel_first.shape[2]
    if cores != 2 or span % 4 or slab % 16 or actions.shape[1] > 7:
        return local_plain(*args)
    nz = span // 4
    buckets = head_weight.shape[2]
    lanes = -(-(buckets + 1) // 128) * 128
    half = kernel_first.shape[3]

    used = gather_call(
        nz,
        lanes,
        kernel_first.reshape(9, slab, half),
        kernel_second.reshape(9, slab, half),
        head_weight,
        action_embed,
    )
    count = hidden_state.shape[0] // cores
    begin = lax.axis_index("mp") * count

    used, hidden_state = lax.optimization_barrier((tuple(used), hidden_state))
    states = lax.dynamic_slice_in_dim(hidden_state, begin, count, 0)
    flat = [u.reshape((2, span) + u.shape[4:]) for u in used]
    parts = step_call(
        hidden_state.shape[0] * span, hidden_state.shape[1], buckets,
        actions, value_target, reward_target, states, *flat,
    )
    sums = reduce_call(nz, [p.reshape(u.shape) for p, u in zip(parts, used)])
    def flatten(array):
        return array.reshape(9, slab, half)

    outs = adam_call(
        buckets,
        *sums,
        *[flatten(a) for a in (kernel_first, first_mean, first_square)],
        *[flatten(a) for a in (kernel_second, second_mean, second_square)],
        head_weight, head_mean, head_square,
        action_embed, embed_mean, embed_square,
    )
    shaped = [o.reshape(kernel_first.shape) if o.ndim == 3 and o.shape[0] == 9 else o for o in outs]
    first, second, head, embed = (shaped[4 * i : 4 * i + 4] for i in range(4))
    return (
        first[0], second[0], head[0], embed[0],
        first[1], first[2], second[1], second[2],
        head[1], head[2], embed[1], embed[2],
        first[3], second[3], head[3], embed[3],
    )


def adam_kernel(buckets, *refs):
    sums, old, new = refs[:3], refs[3:15], refs[15:]
    slab = sums[2].shape[1]
    eye = lax.broadcasted_iota(jnp.int32, (slab, slab), 0) == lax.broadcasted_iota(
        jnp.int32, (slab, slab), 1
    )
    embed_grad = jnp.sum(
        jnp.where(eye, sums[2][0, :, buckets : buckets + 1], 0.0), axis=0, keepdims=True
    )
    grads = (sums[0][...], sums[1][...], sums[2][:, :, :buckets], embed_grad)
    for i, grad in enumerate(grads):
        param, mean, square = (old[3 * i + j][...] for j in range(3))
        made = adam_update(param, grad, mean, square) + (grad,)
        for j in range(4):
            new[4 * i + j][...] = made[j]


def adam_call(buckets, *arrays):
    vmem = pl.BlockSpec(memory_space=pltpu.VMEM)
    shapes = []
    for i in range(4):
        shapes += [jax.ShapeDtypeStruct(arrays[3 + 3 * i].shape, jnp.float32)] * 4
    return pl.pallas_call(
        functools.partial(adam_kernel, buckets),
        out_shape=shapes,
        in_specs=[vmem] * len(arrays),
        out_specs=[vmem] * len(shapes),
        name="adam",
    )(*arrays)


def solution(mesh):
    placed = (
        P("dp", None, None, None),
        P("dp", None),
        P("dp", None),
        P("dp", None),
        P(None, None, "dp", "mp"),
        P(None, None, "dp", "mp"),
        P("mp", "dp", None),
        P("mp", "dp"),
        P(None, None, "dp", "mp"),
        P(None, None, "dp", "mp"),
        P(None, None, "dp", "mp"),
        P(None, None, "dp", "mp"),
        P("mp", "dp", None),
        P("mp", "dp", None),
        P("mp", "dp"),
        P("mp", "dp"),
    )
    return jax.shard_map(
        local,
        mesh=mesh,
        in_specs=placed,
        out_specs=(
            P(None, None, "dp", "mp"),
            P(None, None, "dp", "mp"),
            P("mp", "dp", None),
            P("mp", "dp"),
            P(None, None, "dp", "mp"),
            P(None, None, "dp", "mp"),
            P(None, None, "dp", "mp"),
            P(None, None, "dp", "mp"),
            P("mp", "dp", None),
            P("mp", "dp", None),
            P("mp", "dp"),
            P("mp", "dp"),
            P(None, None, "dp", "mp"),
            P(None, None, "dp", "mp"),
            P("mp", "dp", None),
            P("mp", "dp"),
        ),
        check_vma=False,
    )
```
